32 devices in a mesh: dp: 8 (over z, x), tensor: 4 (over y, core).
Axes of the slice: x: 2, y: 2, z: 4, core: 2. Of those that a mesh axis runs over, the one named last changes fastest.
Arguments:
- tokens: bfloat16 [8, 1024, 1152], P('dp', 'tensor'), may hold values from -6 to 6
- modulation: float32 [8, 6, 1152], P('dp'), may hold values from -4 to 4
- qkv_weight: bfloat16 [1152, 3, 1152], P(None, None, 'tensor'), may hold values from -0.1875 to 0.1875
- qv_bias: bfloat16 [2, 1152], P(None, 'tensor'), may hold values from -3 to 3
- out_weight: bfloat16 [1152, 1152], P('tensor'), may hold values from -1.5 to 1.5
- out_bias: bfloat16 [1152], replicated, may hold values from -3 to 3
- up_weight: bfloat16 [1152, 4608], P(None, 'tensor'), may hold values from -0.1875 to 0.1875
- up_bias: bfloat16 [4608], P('tensor'), may hold values from -3 to 3
- down_weight: bfloat16 [4608, 1152], P('tensor'), may hold values from -0.09375 to 0.09375
- down_bias: bfloat16 [1152], replicated, may hold values from -3 to 3
- cotangent: bfloat16 [8, 1024, 1152], P('dp', 'tensor'), may hold values from -6 to 6
- qkv_factor: float32 [3, 1152, 8], P(None, 'tensor'), may hold values from -6 to 6
- out_factor: float32 [1152, 8], P('tensor'), may hold values from -6 to 6
- up_factor: float32 [4608, 8], P('tensor'), may hold values from -6 to 6
- down_factor: float32 [4608, 8], P('tensor'), may hold values from -6 to 6
- qkv_error: float32 [8, 1152, 3, 1152], P('dp', None, None, 'tensor'), may hold values from -24 to 24
- out_error: float32 [8, 1152, 1152], P('dp', 'tensor'), may hold values from -24 to 24
- up_error: float32 [8, 1152, 4608], P('dp', None, 'tensor'), may hold values from -24 to 24
- down_error: float32 [8, 4608, 1152], P('dp', 'tensor'), may hold values from -24 to 24
- qkv_moment: float32 [1152, 3, 1152], P('dp', None, 'tensor'), may hold values from -18 to 18
- out_moment: float32 [1152, 1152], P('tensor', 'dp'), may hold values from -18 to 18
- up_moment: float32 [1152, 4608], P('dp', 'tensor'), may hold values from -18 to 18
- down_moment: float32 [4608, 1152], P('tensor', 'dp'), may hold values from -18 to 18
- qvbias_moment: float32 [2, 1152], P(None, 'tensor'), may hold values from -18 to 18
- outbias_moment: float32 [1152], replicated, may hold values from -18 to 18
- upbias_moment: float32 [4608], P('tensor'), may hold values from -18 to 18
- downbias_moment: float32 [1152], replicated, may hold values from -18 to 18
Outputs:
- tokens_out: bfloat16 [8, 1024, 1152], P('dp', 'tensor')
- tokens_grad: float32 [8, 1024, 1152], P('dp', 'tensor')
- modulation_grad: float32 [8, 6, 1152], P('dp')
- qkv_factor_next: float32 [3, 1152, 8], P(None, 'tensor')
- qkv_error_next: float32 [8, 1152, 3, 1152], P('dp', None, None, 'tensor')
- qkv_moment_next: float32 [1152, 3, 1152], P('dp', None, 'tensor')
- qkv_update: float32 [1152, 3, 1152], P('dp', None, 'tensor')
- out_factor_next: float32 [1152, 8], P('tensor')
- out_error_next: float32 [8, 1152, 1152], P('dp', 'tensor')
- out_moment_next: float32 [1152, 1152], P('tensor', 'dp')
- out_update: float32 [1152, 1152], P('tensor', 'dp')
- up_factor_next: float32 [4608, 8], P('tensor')
- up_error_next: float32 [8, 1152, 4608], P('dp', None, 'tensor')
- up_moment_next: float32 [1152, 4608], P('dp', 'tensor')
- up_update: float32 [1152, 4608], P('dp', 'tensor')
- down_factor_next: float32 [4608, 8], P('tensor')
- down_error_next: float32 [8, 4608, 1152], P('dp', 'tensor')
- down_moment_next: float32 [4608, 1152], P('tensor', 'dp')
- down_update: float32 [4608, 1152], P('tensor', 'dp')
- qvbias_moment_next: float32 [2, 1152], P(None, 'tensor')
- qvbias_update: float32 [2, 1152], P(None, 'tensor')
- outbias_moment_next: float32 [1152], replicated
- outbias_update: float32 [1152], replicated
- upbias_moment_next: float32 [4608], P('tensor')
- upbias_update: float32 [4608], P('tensor')
- downbias_moment_next: float32 [1152], replicated
- downbias_update: float32 [1152], replicated
The draws below stay inside these ranges and needn't reach their ends.
All inputs are finite; a program needn't handle non-finite values.
Results may differ from the reference program's by a relative error of at most 0.023.
The reference program's roundings to bfloat16 on the way count: a program that leaves them out, or rounds other values in their place, can miss the bound.
Values may be sent and summed in bfloat16 or wider, within the bound.
A program may use at most 128 MiB of HBM per device.

```python
import jax
import jax.numpy as jnp
from jax import lax

D = 1152
HEADS = 16
HEAD = 72
FF = 4608
SEQ = 1024
RANK = 8
LAT_DEV = 1
LATENTS = 8
N_DP = 8
N_TENSOR = 4


def with_spikes(values, rng, source, target, parts, factor):
    owner, partner = [(jnp.arange(values.shape[axis_at]) // (values.shape[axis_at] // parts)).reshape([-1 if axis == axis_at else 1 for axis in range(values.ndim)]) for axis_at in (source, target)]
    chosen = jax.random.permutation(rng, parts)[partner]
    strong = (owner == chosen) | (owner == (partner + parts // 2) % parts)
    return jnp.where(strong, factor * values, values)


def block_levels(stream_key, shape, shards, low, top_value):
    def one(axis_at, shards_of):
        steps = jax.random.uniform(jax.random.fold_in(jax.random.fold_in(stream_key, 6), axis_at), (shards_of,), jnp.float32, low / len(shards), top_value / len(shards))
        return jnp.repeat(jnp.exp(steps), shape[axis_at] // shards_of).reshape((-1,) + (1,) * (len(shape) - axis_at - 1))

    loudness = one(*shards[0])
    for cut in shards[1:]:
        loudness = loudness * one(*cut)
    return loudness


def noise(key, extent, scale, reach, cuts=(), kind=jnp.bfloat16):
    gain = block_levels(key, extent, cuts, -0.22, 0.18) if cuts else 1.0
    values = jax.random.normal(key, extent, jnp.float32) * scale * gain
    return jnp.minimum(jnp.maximum(values, -reach), reach).astype(kind)


def noise_with(key, shape, scale, most, cuts, heavy, held_as=jnp.bfloat16):
    values = scale * jax.random.normal(key, shape, jnp.float32)
    if cuts:
        values = values * block_levels(key, shape, cuts, -0.22, 0.18)
    return jnp.clip(with_spikes(values, jax.random.fold_in(key, 3), *heavy), -most, most).astype(held_as)


def setup_inputs(seed: int = 0) -> dict:
    seeds = jax.random.split(jax.random.key(seed), 28)
    return {
        "tokens": noise(seeds[0], (LATENTS, SEQ, D), 1.0, 6.0, ((0, 8), (1, 4))),
        "modulation": noise(seeds[1], (LATENTS, 6, D), 1.0, 4.0, ((0, 8),), jnp.float32),
        "qkv_weight": noise(seeds[2], (D, 3, D), D ** -0.5, 0.1875, ((2, 4),)),
        "qv_bias": noise(seeds[3], (2, D), 0.5, 3.0, ((1, 4),)),
        "out_weight": noise(seeds[4], (D, D), (D // 64) ** -0.5, 1.5, ((0, 4),)),
        "out_bias": noise(seeds[5], (D,), 0.5, 3.0),
        "up_weight": noise(seeds[6], (D, FF), D ** -0.5, 0.1875, ((1, 4),)),
        "up_bias": noise(seeds[7], (FF,), 0.5, 3.0, ((0, 4),)),
        "down_weight": noise(seeds[8], (FF, D), FF ** -0.5, 0.09375, ((0, 4),)),
        "down_bias": noise(seeds[9], (D,), 0.5, 3.0),
        "cotangent": noise(seeds[10], (LATENTS, SEQ, D), 1.0, 6.0, ((0, 8), (1, 4))),
        "qkv_factor": noise(seeds[11], (3, D, RANK), 1.0, 6.0, ((1, 4),), jnp.float32),
        "out_factor": noise(seeds[12], (D, RANK), 1.0, 6.0, ((0, 4),), jnp.float32),
        "up_factor": noise(seeds[13], (FF, RANK), 1.0, 6.0, ((0, 4),), jnp.float32),
        "down_factor": noise(seeds[14], (FF, RANK), 1.0, 6.0, ((0, 4),), jnp.float32),
        "qkv_error": noise_with(seeds[15], (N_DP, D, 3, D), 4.0, 24.0, ((0, 8), (3, 4)), (0, 1, 8, 2.0), jnp.float32),
        "out_error": noise_with(seeds[16], (N_DP, D, D), 4.0, 24.0, ((0, 8), (1, 4)), (0, 2, 8, 2.0), jnp.float32),
        "up_error": noise_with(seeds[17], (N_DP, D, FF), 4.0, 24.0, ((0, 8), (2, 4)), (0, 1, 8, 2.0), jnp.float32),
        "down_error": noise_with(seeds[18], (N_DP, FF, D), 4.0, 24.0, ((0, 8), (1, 4)), (0, 2, 8, 2.0), jnp.float32),
        "qkv_moment": noise(seeds[19], (D, 3, D), 3.0, 18.0, ((0, 8), (2, 4)), jnp.float32),
        "out_moment": noise(seeds[20], (D, D), 3.0, 18.0, ((0, 4), (1, 8)), jnp.float32),
        "up_moment": noise(seeds[21], (D, FF), 3.0, 18.0, ((0, 8), (1, 4)), jnp.float32),
        "down_moment": noise(seeds[22], (FF, D), 3.0, 18.0, ((0, 4), (1, 8)), jnp.float32),
        "qvbias_moment": noise(seeds[23], (2, D), 3.0, 18.0, ((1, 4),), jnp.float32),
        "outbias_moment": noise(seeds[24], (D,), 3.0, 18.0, (), jnp.float32),
        "upbias_moment": noise(seeds[25], (FF,), 3.0, 18.0, ((0, 4),), jnp.float32),
        "downbias_moment": noise(seeds[26], (D,), 3.0, 18.0, (), jnp.float32),
    }


EPS = 1e-06
ORTH_EPS = 1e-06
MOMENTUM = 0.9
RATE = 0.01
HIGH = lax.Precision.HIGHEST

@jax.custom_vjp
def low(v):
    return lax.optimization_barrier(v.astype(jnp.bfloat16)).astype(jnp.float32)

@jax.custom_vjp
def low_back(v):
    return v

def low_keep(v):
    return (low(v), None)

def low_pass(kept, grad):
    return (grad,)

def back_keep(v):
    return (v, None)

def back_low(kept, grad):
    return (low(grad),)
low.defvjp(low_keep, low_pass)
low_back.defvjp(back_keep, back_low)

def layer_norm(values):
    center = values - lax.optimization_barrier(jnp.mean(values, axis=-1, keepdims=True))
    spread = lax.optimization_barrier(jnp.mean(center * center, axis=-1, keepdims=True))
    return center * lax.rsqrt(spread + EPS)

def attend(queries, keyset, valueset):
    scores = low_back(jnp.einsum('qhe,khe->hqk', queries, keyset, precision=HIGH) * HEAD ** (-0.5))
    attn_probs = low(jax.nn.softmax(scores, axis=-1))
    return jnp.einsum('hqk,khe->qhe', attn_probs, valueset, precision=HIGH)

def block(params, tokens, modulation):
    qkv_weight, qv_bias, out_weight, out_bias, up_weight, up_bias, down_weight, down_bias = params
    shift_one = modulation[0]
    scale_one = modulation[1]
    gate_one = modulation[2]
    shift_two = modulation[3]
    scale_two = modulation[4]
    gate_two = modulation[5]
    attn_in = low(layer_norm(tokens) * (1.0 + scale_one) + shift_one)
    projected = jnp.einsum('sd,dtf->stf', attn_in, qkv_weight, precision=HIGH)
    bias_rows = jnp.stack([qv_bias[0], jnp.zeros_like(qv_bias[0]), qv_bias[1]])
    projected = low_back(low(projected + bias_rows))
    queries = projected[:, 0].reshape(SEQ, HEADS, HEAD)
    keyset = projected[:, 1].reshape(SEQ, HEADS, HEAD)
    valueset = projected[:, 2].reshape(SEQ, HEADS, HEAD)
    attn_mix = jax.checkpoint(attend)(queries, keyset, valueset).reshape(SEQ, D)
    attn_mix = low_back(low(attn_mix))
    attn_out = low_back(jnp.dot(attn_mix, out_weight, precision=HIGH) + out_bias)
    middle = tokens + gate_one * attn_out
    mlp_in = low(layer_norm(middle) * (1.0 + scale_two) + shift_two)
    hidden = low_back(jnp.dot(mlp_in, up_weight, precision=HIGH) + up_bias)
    active = low(jax.nn.gelu(hidden, approximate=True))
    mlp_out = low_back(jnp.dot(active, down_weight, precision=HIGH) + down_bias)
    return middle + gate_two * mlp_out

def group_pass(params, tokens, modulation, cotangent):

    def run(params, tokens, modulation):
        return lax.map(lambda pair: block(params, pair[0], pair[1]), (tokens, modulation))
    result, pull = jax.vjp(run, params, tokens, modulation)
    grad_params, grad_tokens, grad_mod = pull(cotangent)
    return (result, grad_params, grad_tokens, grad_mod)

def orthonormal(matrix):
    columns = []
    for column in range(matrix.shape[1]):
        vector = matrix[:, column]
        for previous in columns:
            vector = vector - jnp.sum(previous * vector) * previous
        vector = vector * lax.rsqrt(jnp.sum(vector * vector) + ORTH_EPS)
        columns.append(vector)
    return jnp.stack(columns, axis=1)

def compress(grads, errors, factor):
    corrected = grads + errors
    first_factor = jnp.einsum('itkl,tlr->tkr', corrected, factor, precision=HIGH)
    orthogonal = jax.vmap(orthonormal)(first_factor)
    second = jnp.einsum('itkl,tkr->tlr', corrected, orthogonal, precision=HIGH) / N_DP
    approx = jnp.einsum('tkr,tlr->tkl', orthogonal, second, precision=HIGH)
    return (second, approx, corrected - approx[None])

def qkv_split(array):
    leading = array.shape[0]
    width_here = D // N_TENSOR
    return array.reshape(leading, D, 3, N_TENSOR, width_here).transpose(0, 3, 1, 2, 4).reshape(leading, N_TENSOR, D, 3 * width_here)

def qkv_join(array):
    leading = array.shape[0]
    width_here = D // N_TENSOR
    return array.reshape(leading, N_TENSOR, D, 3, width_here).transpose(0, 2, 3, 1, 4).reshape(leading, D, 3, D)

def rows_split(array):
    leading = array.shape[0]
    return array.reshape(leading, N_TENSOR, array.shape[1] // N_TENSOR, array.shape[2]).transpose(0, 1, 3, 2)

def rows_join(array):
    leading = array.shape[0]
    return array.transpose(0, 1, 3, 2).reshape(leading, N_TENSOR * array.shape[3], array.shape[2])

def cols_split(array):
    leading = array.shape[0]
    return array.reshape(leading, array.shape[1], N_TENSOR, array.shape[2] // N_TENSOR).transpose(0, 2, 1, 3)

def cols_join(array):
    leading = array.shape[0]
    return array.transpose(0, 2, 1, 3).reshape(leading, array.shape[2], N_TENSOR * array.shape[3])

def qkv_factor_split(factor):
    width_here = D // N_TENSOR
    return factor.reshape(3, N_TENSOR, width_here, RANK).transpose(1, 0, 2, 3).reshape(N_TENSOR, 3 * width_here, RANK)

def qkv_factor_join(factor):
    width_here = D // N_TENSOR
    return factor.reshape(N_TENSOR, 3, width_here, RANK).transpose(1, 0, 2, 3).reshape(3, D, RANK)

def powered(grads, errors, factor, split, join):
    second, approx, error_next = compress(split(grads), split(errors), factor)
    return (second, join(approx[None])[0], join(error_next))

def advance(moment, grad):
    moment_next = MOMENTUM * moment + grad
    return (moment_next, -RATE * (grad + MOMENTUM * moment_next))

def reference(tokens, modulation, qkv_weight, qv_bias, out_weight, out_bias, up_weight, up_bias, down_weight, down_bias, cotangent, qkv_factor, out_factor, up_factor, down_factor, qkv_error, out_error, up_error, down_error, qkv_moment, out_moment, up_moment, down_moment, qvbias_moment, outbias_moment, upbias_moment, downbias_moment):
    params = tuple((weight.astype(jnp.float32) for weight in (qkv_weight, qv_bias, out_weight, out_bias, up_weight, up_bias, down_weight, down_bias)))
    token_groups = tokens.astype(jnp.float32).reshape(N_DP, LAT_DEV, SEQ, D)
    mod_groups = modulation.reshape(N_DP, LAT_DEV, 6, D)
    cot_groups = cotangent.astype(jnp.float32).reshape(N_DP, LAT_DEV, SEQ, D)
    outputs, grads, token_grads, mod_grads = lax.map(lambda group: group_pass(params, group[0], group[1], group[2]), (token_groups, mod_groups, cot_groups))
    tokens_out = outputs.reshape(LATENTS, SEQ, D).astype(jnp.bfloat16)
    tokens_grad = token_grads.reshape(LATENTS, SEQ, D)
    modulation_grad = mod_grads.reshape(LATENTS, 6, D)
    qkv_second, qkv_approx, qkv_error_next = powered(grads[0], qkv_error, qkv_factor_split(qkv_factor), qkv_split, qkv_join)
    out_second, out_approx, out_error_next = powered(grads[2], out_error, out_factor.reshape(N_TENSOR, -1, RANK), rows_split, rows_join)
    up_second, up_approx, up_error_next = powered(grads[4], up_error, up_factor.reshape(N_TENSOR, -1, RANK), cols_split, cols_join)
    down_second, down_approx, down_error_next = powered(grads[6], down_error, down_factor.reshape(N_TENSOR, -1, RANK), rows_split, rows_join)
    qkv_moment_next, qkv_update = advance(qkv_moment, qkv_approx)
    out_moment_next, out_update = advance(out_moment, out_approx)
    up_moment_next, up_update = advance(up_moment, up_approx)
    down_moment_next, down_update = advance(down_moment, down_approx)
    qvbias_moment_next, qvbias_update = advance(qvbias_moment, lax.optimization_barrier(jnp.sum(grads[1], axis=0)) / N_DP)
    outbias_moment_next, outbias_update = advance(outbias_moment, lax.optimization_barrier(jnp.sum(grads[3], axis=0)) / N_DP)
    upbias_moment_next, upbias_update = advance(upbias_moment, lax.optimization_barrier(jnp.sum(grads[5], axis=0)) / N_DP)
    downbias_moment_next, downbias_update = advance(downbias_moment, lax.optimization_barrier(jnp.sum(grads[7], axis=0)) / N_DP)
    return (tokens_out, tokens_grad, modulation_grad, qkv_factor_join(qkv_second), qkv_error_next, qkv_moment_next, qkv_update, out_second.reshape(D, RANK), out_error_next, out_moment_next, out_update, up_second.reshape(FF, RANK), up_error_next, up_moment_next, up_update, down_second.reshape(FF, RANK), down_error_next, down_moment_next, down_update, qvbias_moment_next, qvbias_update, outbias_moment_next, outbias_update, upbias_moment_next, upbias_update, downbias_moment_next, downbias_update)
```

```python
import functools

import jax
import jax.numpy as jnp
from jax import lax
from jax.experimental import pallas as pl
from jax.experimental.pallas import tpu as pltpu
from jax.sharding import PartitionSpec as P

HEAD = 72
RANK = 8
EPS = 1e-06
ORTH_EPS = 1e-06
MOMENTUM = 0.9
RATE = 0.01
HIGH = lax.Precision.HIGHEST
F32 = jnp.float32
BF16 = jnp.bfloat16
MESH = pl.DeviceIdType.MESH
VMEM_LIMIT = 60 * 1024 * 1024
LOG2E = 1.4426950408889634
GELU_C = 0.7978845608028654


def dot_nn(a, b):
    return lax.dot_general(a, b, (((1,), (0,)), ((), ())), preferred_element_type=F32)


def dot_nt(a, b):
    return lax.dot_general(a, b, (((1,), (1,)), ((), ())), preferred_element_type=F32)


def dot_tn(a, b):
    return lax.dot_general(a, b, (((0,), (0,)), ((), ())), preferred_element_type=F32)


def split_low(value):
    high = value.astype(BF16)
    return high, (value - high.astype(F32)).astype(BF16)


def cost(flops, nbytes, trans=0):
    return pl.CostEstimate(flops=int(flops), bytes_accessed=int(nbytes), transcendentals=int(trans))


def swap(value, bit):
    size = lax.axis_size("tensor")
    return lax.ppermute(value, "tensor", [(i, i ^ bit) for i in range(size)])


def gather_halves(own):
    beside = swap(own, 1)
    across = swap(own, 2)
    corner = swap(across, 1)
    return jnp.concatenate([own, beside], axis=0), jnp.concatenate([across, corner], axis=0)


def far_sum(far_part, rows):
    joined = swap(far_part[rows:], 1)
    chip_sum = (far_part[:rows].astype(F32) + joined.astype(F32)).astype(BF16)
    return swap(chip_sum, 2)


def near_sum(near_part, rows):
    return near_part[:rows].astype(F32) + swap(near_part[rows:], 1).astype(F32)


def attn_fwd_kernel(use_far, heads, near_ref, far_ref, mix_ref, lse_ref):
    width = heads * HEAD
    scale = HEAD ** (-0.5)
    half = near_ref.shape[0]
    block = 256
    q_ref = far_ref if use_far else near_ref
    for h in range(heads):
        cols = slice(h * HEAD, (h + 1) * HEAD)
        kcols = slice(width + h * HEAD, width + (h + 1) * HEAD)
        vcols = slice(2 * width + h * HEAD, 2 * width + (h + 1) * HEAD)
        keys = jnp.concatenate([near_ref[:, kcols], far_ref[:, kcols]], axis=0)
        values_t = jnp.concatenate([near_ref[:, vcols], far_ref[:, vcols]], axis=0).T
        for b in range(half // block):
            rows = slice(b * block, (b + 1) * block)
            scores = dot_nt(keys, q_ref[rows, cols])
            top = jnp.max(scores, axis=0, keepdims=True)
            expd = jnp.exp2((scores - top) * (scale * LOG2E))
            total = jnp.sum(expd, axis=0, keepdims=True)
            probs = (expd * (1.0 / total)).astype(BF16)
            mixed = dot_nn(values_t, probs)
            mix_ref[rows, cols] = mixed.T.astype(BF16)
            lse_ref[h : h + 1, rows] = top * (scale * LOG2E) + jnp.log2(total)


def attn_fwd(near, far, use_far, heads):
    half = near.shape[0]
    width = heads * HEAD
    return pl.pallas_call(
        functools.partial(attn_fwd_kernel, use_far, heads),
        out_shape=(
            jax.ShapeDtypeStruct((half, width), BF16),
            jax.ShapeDtypeStruct((heads, half), F32),
        ),
        in_specs=[pl.BlockSpec(memory_space=pltpu.VMEM)] * 2,
        out_specs=[pl.BlockSpec(memory_space=pltpu.VMEM)] * 2,
        compiler_params=pltpu.CompilerParams(vmem_limit_bytes=VMEM_LIMIT),
        cost_estimate=cost(8 * heads * half * half * 128 * 2, 8 * half * width, 2 * heads * half * half),
        name="attn_fwd",
    )(near, far)


def attn_bwd_kernel(last, heads, near_ref, far_ref, lse_ref, gmix_ref, *rest):
    width = heads * HEAD
    scale = HEAD ** (-0.5)
    half = near_ref.shape[0]
    length = 2 * half
    block = 256
    if last:
        dq_ref, acck_ref, accv_ref, gnear_ref, gfar_ref = rest
        q_ref = far_ref
    else:
        dqo_ref, dk_ref, dv_ref = rest
        q_ref = near_ref
    for h in range(heads):
        cols = slice(h * HEAD, (h + 1) * HEAD)
        kcols = slice(width + h * HEAD, width + (h + 1) * HEAD)
        vcols = slice(2 * width + h * HEAD, 2 * width + (h + 1) * HEAD)
        keys = jnp.concatenate([near_ref[:, kcols], far_ref[:, kcols]], axis=0)
        values = jnp.concatenate([near_ref[:, vcols], far_ref[:, vcols]], axis=0)
        keys_t = keys.T
        dkey = jnp.zeros((length, HEAD), F32)
        dvalue = jnp.zeros((length, HEAD), F32)
        for b in range(half // block):
            rows = slice(b * block, (b + 1) * block)
            q = q_ref[rows, cols]
            gmix = gmix_ref[rows, cols]
            scores = dot_nt(keys, q)
            probs = jnp.exp2(scores * (scale * LOG2E) - lse_ref[h : h + 1, rows])
            gprobs = dot_nt(values, gmix)
            inner = jnp.sum(probs * gprobs, axis=0, keepdims=True)
            gscores = (probs * (gprobs - inner)).astype(BF16)
            dvalue = dvalue + dot_nn(probs.astype(BF16), gmix)
            dkey = dkey + dot_nn(gscores, q)
            dquery = (dot_nn(keys_t, gscores) * scale).T.astype(BF16)
            if last:
                gfar_ref[rows, cols] = dquery
            else:
                dqo_ref[rows, cols] = dquery
        if last:
            dkey = ((dkey + acck_ref[h]) * scale).astype(BF16)
            dvalue = (dvalue + accv_ref[h]).astype(BF16)
            gnear_ref[:, kcols] = dkey[:half]
            gfar_ref[:, kcols] = dkey[half:]
            gnear_ref[:, vcols] = dvalue[:half]
            gfar_ref[:, vcols] = dvalue[half:]
        else:
            dk_ref[h] = dkey
            dv_ref[h] = dvalue
    if last:
        gnear_ref[:, :width] = dq_ref[...]


def attn_bwd(near, far, lse, gmix, heads, carried=None):
    half = near.shape[0]
    width = heads * HEAD
    last = carried is not None
    if last:
        out_shape = (jax.ShapeDtypeStruct((half, 3 * width), BF16),) * 2
    else:
        out_shape = (
            jax.ShapeDtypeStruct((half, width), BF16),
            jax.ShapeDtypeStruct((heads, 2 * half, HEAD), F32),
            jax.ShapeDtypeStruct((heads, 2 * half, HEAD), F32),
        )
    operands = (near, far, lse, gmix) + (tuple(carried) if last else ())
    return pl.pallas_call(
        functools.partial(attn_bwd_kernel, last, heads),
        out_shape=out_shape,
        in_specs=[pl.BlockSpec(memory_space=pltpu.VMEM)] * len(operands),
        out_specs=[pl.BlockSpec(memory_space=pltpu.VMEM)] * len(out_shape),
        compiler_params=pltpu.CompilerParams(vmem_limit_bytes=VMEM_LIMIT),
        cost_estimate=cost(20 * heads * half * half * 128 * 2, 20 * half * width, 2 * heads * half * half),
        name="attn_bwd",
    )(*operands)


def mlp_kernel(x_ref, g_ref, up_ref, bias_ref, down_ref, act_ref, ghid_ref, down_part_ref, in_part_ref):
    hidden = dot_nn(x_ref[...], up_ref[...]) + bias_ref[...]
    square = hidden * hidden
    tanh = jnp.tanh(GELU_C * hidden * (1.0 + 0.044715 * square))
    half_plus = 0.5 + 0.5 * tanh
    active = (hidden * half_plus).astype(BF16)
    slope = half_plus + 0.5 * hidden * (1.0 - tanh * tanh) * (GELU_C + (3.0 * 0.044715 * GELU_C) * square)
    act_ref[...] = active
    down_part_ref[...] = dot_nn(active, down_ref[...]).astype(BF16)
    ghid = (dot_nt(g_ref[...], down_ref[...]) * slope).astype(BF16)
    ghid_ref[...] = ghid
    in_part_ref[...] = dot_nt(ghid, up_ref[...]).astype(BF16)


def mlp(x, g, up, bias, down):
    half, width = x.shape
    hid = up.shape[1]
    block = 256
    row = lambda i: (i, 0)
    fixed = lambda i: (0, 0)
    return pl.pallas_call(
        mlp_kernel,
        out_shape=(
            jax.ShapeDtypeStruct((half, hid), BF16),
            jax.ShapeDtypeStruct((half, hid), BF16),
            jax.ShapeDtypeStruct((half, width), BF16),
            jax.ShapeDtypeStruct((half, width), BF16),
        ),
        grid=(half // block,),
        in_specs=[
            pl.BlockSpec((block, width), row),
            pl.BlockSpec((block, width), row),
            pl.BlockSpec((width, hid), fixed, pipeline_mode=pl.Buffered(1)),
            pl.BlockSpec((1, hid), fixed, pipeline_mode=pl.Buffered(1)),
            pl.BlockSpec((hid, width), fixed, pipeline_mode=pl.Buffered(1)),
        ],
        out_specs=[
            pl.BlockSpec((block, hid), row),
            pl.BlockSpec((block, hid), row),
            pl.BlockSpec((block, width), row),
            pl.BlockSpec((block, width), row),
        ],
        compiler_params=pltpu.CompilerParams(vmem_limit_bytes=VMEM_LIMIT),
        cost_estimate=cost(8 * half * width * hid, 12 * half * width + 4 * width * hid, half * hid),
        name="mlp",
    )(x, g, up, bias, down)


def grad_kernel(by_rows, an_ref, af_ref, bn_ref, bf_ref, err_ref, qt_ref, mat_ref, left_ref, bias_ref):
    step = pl.program_id(0)
    grad = dot_tn(an_ref[...], bn_ref[...]) + dot_tn(af_ref[...], bf_ref[...])
    mat = grad + err_ref[...]
    mat_ref[...] = mat
    high, low = split_low(mat)
    q_high, q_low = split_low(qt_ref[...])
    if by_rows:
        left_ref[...] = dot_nt(q_high, high) + (dot_nt(q_low, high) + dot_nt(q_high, low))
    else:
        part = dot_nn(q_high, high) + (dot_nn(q_low, high) + dot_nn(q_high, low))

        @pl.when(step == 0)
        def _():
            left_ref[...] = part

        @pl.when(step > 0)
        def _():
            left_ref[...] += part

    @pl.when(step == 0)
    def _():
        ones = jnp.ones((8, bn_ref.shape[0]), BF16)
        bias_ref[...] = dot_nn(ones, bn_ref[...]) + dot_nn(ones, bf_ref[...])


def weight_grad(a_near, a_far, b_near, b_far, error, factor_t, by_rows, block):
    half, rows = a_near.shape
    cols = b_near.shape[1]
    rank = factor_t.shape[0]
    fixed = lambda i: (0, 0)
    row = lambda i: (i, 0)
    col = lambda i: (0, i)
    if by_rows:
        left_len, left_spec = rows, pl.BlockSpec((rank, block), col)
        q_spec = pl.BlockSpec((rank, cols), fixed)
    else:
        left_len, left_spec = cols, pl.BlockSpec((rank, cols), fixed)
        q_spec = pl.BlockSpec((rank, block), col)
    return pl.pallas_call(
        functools.partial(grad_kernel, by_rows),
        out_shape=(
            jax.ShapeDtypeStruct((rows, cols), F32),
            jax.ShapeDtypeStruct((rank, left_len), F32),
            jax.ShapeDtypeStruct((8, cols), F32),
        ),
        grid=(rows // block,),
        in_specs=[
            pl.BlockSpec((half, block), col),
            pl.BlockSpec((half, block), col),
            pl.BlockSpec((half, cols), fixed, pipeline_mode=pl.Buffered(1)),
            pl.BlockSpec((half, cols), fixed, pipeline_mode=pl.Buffered(1)),
            pl.BlockSpec((block, cols), row),
            q_spec,
        ],
        out_specs=[pl.BlockSpec((block, cols), row), left_spec, pl.BlockSpec((8, cols), fixed)],
        compiler_params=pltpu.CompilerParams(vmem_limit_bytes=VMEM_LIMIT),
        cost_estimate=cost(4 * half * rows * cols, 8 * rows * cols + 4 * half * (rows + cols)),
        name="weight_grad",
    )(a_near, a_far, b_near, b_far, error, factor_t)


def orthonormal_rows(work):
    rank = work.shape[0]
    row = lax.broadcasted_iota(jnp.int32, (rank, 1), 0)
    for r in range(rank):
        vector = work[r : r + 1]
        unit = vector * lax.rsqrt(jnp.sum(vector * vector, axis=1, keepdims=True) + ORTH_EPS)
        dots = jnp.sum(work * unit, axis=1, keepdims=True)
        work = jnp.where(row > r, work - dots * unit, work)
        work = jnp.where(row == r, unit, work)
    return work


def pack_three(value, first):
    high = value.astype(BF16).astype(F32)
    low = value - high
    parts = [high, high, low] if first else [high, low, high]
    return jnp.concatenate(parts, axis=0).astype(BF16)


def compress_kernel(
    dp_count,
    kinds,
    rest_block,
    *refs,
):
    count = len(kinds)
    mats = refs[:count]
    lefts = refs[count : 2 * count]
    biases = refs[2 * count : 3 * count]
    outs = refs[3 * count : 7 * count]
    rests, seconds, orthos, bias_outs = (outs[i * count : (i + 1) * count] for i in range(4))
    scratch = refs[7 * count :]
    held = scratch[:count]
    pay_one, got_one, pay_two, got_two, in_sem, out_sem, send_sem, recv_sem = scratch[count:]
    me = lax.axis_index("dp")
    rounds = dp_count.bit_length() - 1

    loads = [pltpu.make_async_copy(mats[i], held[i], in_sem.at[i]) for i in range(count)]
    for load in loads:
        load.start()

    barrier = pltpu.get_barrier_semaphore()
    for k in range(rounds):
        pl.semaphore_signal(barrier, inc=1, device_id={"dp": me ^ (1 << k)}, device_id_type=MESH)

    bias_row = RANK * count
    pay_one[bias_row:] = jnp.zeros_like(pay_one[bias_row:])
    for i in range(count):
        pay_one[RANK * i : RANK * (i + 1)] = lefts[i][...]
        pay_one[bias_row + i : bias_row + i + 1, : biases[i].shape[1]] = biases[i][0:1]
    pl.semaphore_wait(barrier, rounds)

    def all_sum(payload, got, base):
        for k in range(rounds):
            copy = pltpu.make_async_remote_copy(
                src_ref=payload,
                dst_ref=got.at[k],
                send_sem=send_sem.at[base + k],
                recv_sem=recv_sem.at[base + k],
                device_id={"dp": me ^ (1 << k)},
                device_id_type=MESH,
            )
            copy.start()
            copy.wait()
            payload[...] += got[k]

    all_sum(pay_one, got_one, 0)
    for i in range(count):
        bias_outs[i][...] = pay_one[bias_row + i : bias_row + i + 1, : biases[i].shape[1]]
        orthos[i][...] = orthonormal_rows(pay_one[RANK * i : RANK * (i + 1)])

    offsets = []
    where = 0
    for i in range(count):
        offsets.append(where)
        where += seconds[i].shape[1] + (-seconds[i].shape[1]) % 128
    pay_two[...] = jnp.zeros_like(pay_two)
    for i in range(count):
        loads[i].wait()
        rows = held[i].shape[0]
        block = min(rest_block, rows)
        o_high, o_low = split_low(orthos[i][...])
        if kinds[i]:
            total = jnp.zeros((RANK, held[i].shape[1]), F32)
            for b in range(rows // block):
                high, low = split_low(held[i][b * block : (b + 1) * block])
                cut = slice(b * block, (b + 1) * block)
                total += dot_nn(o_high[:, cut], high) + (
                    dot_nn(o_low[:, cut], high) + dot_nn(o_high[:, cut], low)
                )
            pay_two[:, offsets[i] : offsets[i] + held[i].shape[1]] = total
        else:
            for b in range(rows // block):
                high, low = split_low(held[i][b * block : (b + 1) * block])
                part = dot_nt(o_high, high) + (dot_nt(o_low, high) + dot_nt(o_high, low))
                pay_two[:, offsets[i] + b * block : offsets[i] + (b + 1) * block] = part

    all_sum(pay_two, got_two, rounds)

    stores = []
    for i in range(count):
        second = pay_two[:, offsets[i] : offsets[i] + seconds[i].shape[1]] * (1.0 / dp_count)
        seconds[i][...] = second
        rows = held[i].shape[0]
        block = min(rest_block, rows)
        if kinds[i]:
            row_pack, col_pack = pack_three(orthos[i][...], True), pack_three(second, False)
        else:
            row_pack, col_pack = pack_three(second, True), pack_three(orthos[i][...], False)
        for b in range(rows // block):
            cut = slice(b * block, (b + 1) * block)
            held[i][cut] = held[i][cut] - dot_tn(row_pack[:, cut], col_pack)
            store = pltpu.make_async_copy(held[i].at[cut], rests[i].at[cut], out_sem.at[len(stores)])
            store.start()
            stores.append(store)
    for store in stores:
        store.wait()


def compress(mats, lefts, biases, kinds):
    dp_count = lax.axis_size("dp")
    rounds = dp_count.bit_length() - 1
    count = len(mats)
    rest_block = 384
    second_lens = [m.shape[1] if kind else m.shape[0] for m, kind in zip(mats, kinds)]
    wide = sum(n + (-n) % 128 for n in second_lens)
    long = lefts[0].shape[1]
    pay_rows = RANK * count + 8
    pieces = sum(max(1, m.shape[0] // rest_block) for m in mats)
    vm = pl.BlockSpec(memory_space=pltpu.VMEM)
    hbm = pl.BlockSpec(memory_space=pl.ANY)
    return pl.pallas_call(
        functools.partial(compress_kernel, dp_count, kinds, rest_block),
        out_shape=tuple(
            [jax.ShapeDtypeStruct(m.shape, F32) for m in mats]
            + [jax.ShapeDtypeStruct((RANK, n), F32) for n in second_lens]
            + [jax.ShapeDtypeStruct((RANK, long), F32) for _ in mats]
            + [jax.ShapeDtypeStruct((1, b.shape[1]), F32) for b in biases]
        ),
        in_specs=[hbm] * count + [vm] * (2 * count),
        out_specs=[hbm] * count + [vm] * (3 * count),
        scratch_shapes=[pltpu.VMEM(m.shape, F32) for m in mats]
        + [
            pltpu.VMEM((pay_rows, long), F32),
            pltpu.VMEM((rounds, pay_rows, long), F32),
            pltpu.VMEM((RANK, wide), F32),
            pltpu.VMEM((rounds, RANK, wide), F32),
            pltpu.SemaphoreType.DMA((count,)),
            pltpu.SemaphoreType.DMA((pieces,)),
            pltpu.SemaphoreType.DMA((2 * rounds,)),
            pltpu.SemaphoreType.DMA((2 * rounds,)),
        ],
        compiler_params=pltpu.CompilerParams(
            collective_id=1, has_side_effects=True, vmem_limit_bytes=VMEM_LIMIT
        ),
        cost_estimate=cost(4e9, 8 * sum(m.size for m in mats)),
        name="compress",
    )(*mats, *lefts, *biases)


def normalize(values):
    center = values - jnp.mean(values, axis=-1, keepdims=True)
    spread = jnp.mean(center * center, axis=-1, keepdims=True)
    inverse = lax.rsqrt(spread + EPS)
    return center * inverse, inverse


def normalize_back(grad, normed, inverse):
    return inverse * (
        grad
        - jnp.mean(grad, axis=-1, keepdims=True)
        - normed * jnp.mean(grad * normed, axis=-1, keepdims=True)
    )


def advance(moment, grad):
    moment_next = MOMENTUM * moment + grad
    return (moment_next, -RATE * (grad + MOMENTUM * moment_next))


def matmul(a, b, dims):
    return lax.dot_general(a, b, (dims, ((), ())), preferred_element_type=F32)


def per_device(
    tokens,
    modulation,
    qkv_weight,
    qv_bias,
    out_weight,
    out_bias,
    up_weight,
    up_bias,
    down_weight,
    down_bias,
    cotangent,
    qkv_factor,
    out_factor,
    up_factor,
    down_factor,
    qkv_error,
    out_error,
    up_error,
    down_error,
    qkv_moment,
    out_moment,
    up_moment,
    down_moment,
    qvbias_moment,
    outbias_moment,
    upbias_moment,
    downbias_moment,
):
    rows, width = tokens.shape[1:]
    local = qkv_weight.shape[2]
    heads = local // HEAD
    dp_count = lax.axis_size("dp")
    shift_one, scale_one, gate_one, shift_two, scale_two, gate_two = (
        modulation[0, i : i + 1] for i in range(6)
    )
    token_vals = tokens[0].astype(F32)
    grad_final = cotangent[0].astype(F32)
    qkv_flat = qkv_weight.reshape(width, 3 * local)

    normed_one, inverse_one = normalize(token_vals)
    attn_in = (normed_one * (1.0 + scale_one) + shift_one).astype(BF16)
    a_near, a_far = gather_halves(attn_in)
    grad_mlp = (gate_two * grad_final).astype(BF16)
    bias_rows = jnp.concatenate([qv_bias[0], jnp.zeros_like(qv_bias[0]), qv_bias[1]]).astype(F32)
    qkv_near = (matmul(a_near, qkv_flat, ((1,), (0,))) + bias_rows).astype(BF16)
    qkv_far = (matmul(a_far, qkv_flat, ((1,), (0,))) + bias_rows).astype(BF16)
    g_near, g_far = gather_halves(grad_mlp)
    mix_far, lse_far = attn_fwd(qkv_near, qkv_far, True, heads)
    out_far = matmul(mix_far, out_weight, ((1,), (0,))).astype(BF16)
    out_across = far_sum(out_far, rows)
    mix_near, lse_near = attn_fwd(qkv_near, qkv_far, False, heads)
    out_near = matmul(mix_near, out_weight, ((1,), (0,))).astype(BF16)
    attn_out = near_sum(out_near, rows) + out_across.astype(F32) + out_bias.astype(F32)
    middle = token_vals + gate_one * attn_out
    normed_two, inverse_two = normalize(middle)
    mlp_in = (normed_two * (1.0 + scale_two) + shift_two).astype(BF16)
    m_near, m_far = gather_halves(mlp_in)

    up_bias_row = up_bias.astype(F32)[None]
    act_near, ghid_near, down_near, in_near = mlp(m_near, g_near, up_weight, up_bias_row, down_weight)
    act_far, ghid_far, down_far, in_far = mlp(m_far, g_far, up_weight, up_bias_row, down_weight)
    in_across = far_sum(in_far, rows)
    grad_mlp_in = near_sum(in_near, rows) + in_across.astype(F32)
    down_mat, down_left, downb = weight_grad(
        act_near, act_far, g_near, g_far, down_error[0], down_factor.T, False, 384
    )
    up_mat, up_left, upb = weight_grad(
        m_near, m_far, ghid_near, ghid_far, up_error[0], up_factor.T, True, 384
    )
    grad_shift_two = jnp.sum(grad_mlp_in, axis=0)
    grad_scale_two = jnp.sum(grad_mlp_in * normed_two, axis=0)
    grad_middle = grad_final + normalize_back(grad_mlp_in * (1.0 + scale_two), normed_two, inverse_two)
    grad_gate_one = jnp.sum(grad_middle * attn_out, axis=0)
    grad_attn = (gate_one * grad_middle).astype(BF16)
    ga_near, ga_far = gather_halves(grad_attn)

    gmix_near = matmul(ga_near, out_weight, ((1,), (1,))).astype(BF16)
    carried = attn_bwd(qkv_near, qkv_far, lse_near, gmix_near, heads)
    gmix_far = matmul(ga_far, out_weight, ((1,), (1,))).astype(BF16)
    gp_near, gp_far = attn_bwd(qkv_near, qkv_far, lse_far, gmix_far, heads, carried)
    back_far = matmul(gp_far, qkv_flat, ((1,), (1,))).astype(BF16)
    back_across = far_sum(back_far, rows)
    back_near = matmul(gp_near, qkv_flat, ((1,), (1,))).astype(BF16)
    grad_attn_in = near_sum(back_near, rows) + back_across.astype(F32)
    out_mat, out_left, outb = weight_grad(
        mix_near, mix_far, ga_near, ga_far, out_error[0], out_factor.T, False, local
    )
    qkv_mat, qkv_left, qvb = weight_grad(
        a_near,
        a_far,
        gp_near,
        gp_far,
        qkv_error[0].reshape(width, 3 * local),
        qkv_factor.reshape(3 * local, RANK).T,
        True,
        384,
    )

    mlp_across = far_sum(down_far, rows)
    mlp_out = near_sum(down_near, rows) + mlp_across.astype(F32) + down_bias.astype(F32)
    tokens_out = (middle + gate_two * mlp_out).astype(BF16)
    grad_gate_two = jnp.sum(grad_final * mlp_out, axis=0)

    grad_shift_one = jnp.sum(grad_attn_in, axis=0)
    grad_scale_one = jnp.sum(grad_attn_in * normed_one, axis=0)
    tokens_grad = grad_middle + normalize_back(
        grad_attn_in * (1.0 + scale_one), normed_one, inverse_one
    )
    mod_part = jnp.stack(
        [grad_shift_one, grad_scale_one, grad_gate_one, grad_shift_two, grad_scale_two, grad_gate_two]
    )
    mod_part = mod_part + swap(mod_part, 1)
    modulation_grad = mod_part + swap(mod_part, 2)

    kinds = (True, False, True, False)
    result = compress(
        (qkv_mat, out_mat, up_mat, down_mat),
        (qkv_left, out_left, up_left, down_left),
        (qvb, outb, upb, downb),
        kinds,
    )
    rests, seconds, orthos, bias_sums = (result[4 * i : 4 * i + 4] for i in range(4))
    own_rows = width // dp_count
    own_start = lax.axis_index("dp") * own_rows

    def own_grad(i):
        own = lax.dynamic_slice_in_dim(orthos[i], own_start, own_rows, 1)
        pair = (own, seconds[i]) if kinds[i] else (seconds[i], own)
        return jnp.einsum("rk,rl->kl", *pair, precision=HIGH)

    qkv_moment_next, qkv_update = advance(qkv_moment, own_grad(0).reshape(own_rows, 3, local))
    out_moment_next, out_update = advance(out_moment, own_grad(1))
    up_moment_next, up_update = advance(up_moment, own_grad(2))
    down_moment_next, down_update = advance(down_moment, own_grad(3))
    qv_mean = bias_sums[0].reshape(3, local)[0::2] / dp_count
    outb_mean, upb_mean, downb_mean = (bias_sums[i][0] / dp_count for i in (1, 2, 3))
    qvbias_moment_next, qvbias_update = advance(qvbias_moment, qv_mean)
    outbias_moment_next, outbias_update = advance(outbias_moment, outb_mean)
    upbias_moment_next, upbias_update = advance(upbias_moment, upb_mean)
    downbias_moment_next, downbias_update = advance(downbias_moment, downb_mean)
    return (
        tokens_out[None],
        tokens_grad[None],
        modulation_grad[None],
        seconds[0].T.reshape(3, local, RANK),
        rests[0].reshape(1, width, 3, local),
        qkv_moment_next,
        qkv_update,
        seconds[1].T,
        rests[1][None],
        out_moment_next,
        out_update,
        seconds[2].T,
        rests[2][None],
        up_moment_next,
        up_update,
        seconds[3].T,
        rests[3][None],
        down_moment_next,
        down_update,
        qvbias_moment_next,
        qvbias_update,
        outbias_moment_next,
        outbias_update,
        upbias_moment_next,
        upbias_update,
        downbias_moment_next,
        downbias_update,
    )


def solution(mesh):
    placed = (
        P("dp", "tensor", None),
        P("dp", None, None),
        P(None, None, "tensor"),
        P(None, "tensor"),
        P("tensor", None),
        P(),
        P(None, "tensor"),
        P("tensor"),
        P("tensor", None),
        P(),
        P("dp", "tensor", None),
        P(None, "tensor", None),
        P("tensor", None),
        P("tensor", None),
        P("tensor", None),
        P("dp", None, None, "tensor"),
        P("dp", "tensor", None),
        P("dp", None, "tensor"),
        P("dp", "tensor", None),
        P("dp", None, "tensor"),
        P("tensor", "dp"),
        P("dp", "tensor"),
        P("tensor", "dp"),
        P(None, "tensor"),
        P(),
        P("tensor"),
        P(),
    )
    return jax.shard_map(
        per_device,
        mesh=mesh,
        in_specs=placed,
        out_specs=(
            P("dp", "tensor", None),
            P("dp", "tensor", None),
            P("dp", None, None),
            P(None, "tensor", None),
            P("dp", None, None, "tensor"),
            P("dp", None, "tensor"),
            P("dp", None, "tensor"),
            P("tensor", None),
            P("dp", "tensor", None),
            P("tensor", "dp"),
            P("tensor", "dp"),
            P("tensor", None),
            P("dp", None, "tensor"),
            P("dp", "tensor"),
            P("dp", "tensor"),
            P("tensor", None),
            P("dp", "tensor", None),
            P("tensor", "dp"),
            P("tensor", "dp"),
            P(None, "tensor"),
            P(None, "tensor"),
            P(),
            P(),
            P("tensor"),
            P("tensor"),
            P(),
            P(),
        ),
        check_vma=False,
    )
```

```python
import functools

import jax
import jax.numpy as jnp
from jax import lax
from jax.experimental import pallas as pl
from jax.experimental.pallas import tpu as pltpu
from jax.sharding import PartitionSpec as P

HEAD = 72
RANK = 8
EPS = 1e-06
ORTH_EPS = 1e-06
MOMENTUM = 0.9
RATE = 0.01
HIGH = lax.Precision.HIGHEST
F32 = jnp.float32
BF16 = jnp.bfloat16
MESH = pl.DeviceIdType.MESH
VMEM_LIMIT = 60 * 1024 * 1024
LOG2E = 1.4426950408889634
GELU_C = 0.7978845608028654


def dot_nn(a, b):
    return lax.dot_general(a, b, (((1,), (0,)), ((), ())), preferred_element_type=F32)


def dot_nt(a, b):
    return lax.dot_general(a, b, (((1,), (1,)), ((), ())), preferred_element_type=F32)


def dot_tn(a, b):
    return lax.dot_general(a, b, (((0,), (0,)), ((), ())), preferred_element_type=F32)


def split_low(value):
    high = value.astype(BF16)
    return high, (value - high.astype(F32)).astype(BF16)


def cost(flops, nbytes, trans=0):
    return pl.CostEstimate(flops=int(flops), bytes_accessed=int(nbytes), transcendentals=int(trans))


def swap(value, bit):
    size = lax.axis_size("tensor")
    return lax.ppermute(value, "tensor", [(i, i ^ bit) for i in range(size)])


def after(value, *others):
    return lax.optimization_barrier((value, *others))[0]


def chip_sum(part_across, part_corner):
    joined = swap(part_corner, 1)
    return (part_across.astype(F32) + joined.astype(F32)).astype(BF16)


SCALE = HEAD ** (-0.5)
EXP_SCALE = SCALE * LOG2E


def attn_fwd_kernel(heads, first, *refs):
    pieces, (mix_a, mix_b, lse_ref) = refs[:4], refs[4:]
    rows = pieces[0].shape[2]

    def one_head(h, carry):
        keys = jnp.concatenate([p[heads + h] for p in pieces], axis=1).T
        values_t = jnp.concatenate([p[2 * heads + h] for p in pieces], axis=1)
        for b, mix_ref in enumerate((mix_a, mix_b)):
            scores = dot_nn(keys, pieces[first + b][h])
            top = jnp.max(scores, axis=0, keepdims=True)
            expd = jnp.exp2((scores - top) * EXP_SCALE)
            total = jnp.sum(expd, axis=0, keepdims=True)
            probs = (expd * (1.0 / total)).astype(BF16)
            mix_ref[h] = dot_nn(values_t, probs).astype(BF16)
            lse_ref[h, b : b + 1] = top * EXP_SCALE + jnp.log2(total)
        return carry

    lax.fori_loop(0, heads, one_head, 0)


def attn_fwd(pieces, first, heads):
    rows = pieces[0].shape[2]
    vm = pl.BlockSpec(memory_space=pltpu.VMEM)
    return pl.pallas_call(
        functools.partial(attn_fwd_kernel, heads, first),
        out_shape=(
            jax.ShapeDtypeStruct((heads, HEAD, rows), BF16),
            jax.ShapeDtypeStruct((heads, HEAD, rows), BF16),
            jax.ShapeDtypeStruct((heads, 2, rows), F32),
        ),
        in_specs=[vm] * 4,
        out_specs=[vm] * 3,
        compiler_params=pltpu.CompilerParams(vmem_limit_bytes=24 << 20),
        cost_estimate=cost(32 * heads * rows * rows * 128, 16 * rows * heads * HEAD, 8 * heads * rows * rows),
        name="attn_fwd",
    )(*pieces)


def attn_bwd_kernel(heads, first, last, *refs):
    pieces = refs[:4]
    lse_ref, gmix_a, gmix_b = refs[4:7]
    rows = pieces[0].shape[2]
    if last:
        dq_in = refs[7:9]
        acck_ref, accv_ref = refs[9:11]
        outs = refs[11:]
    else:
        dq_outs = refs[7:9]
        dk_ref, dv_ref = refs[9:11]

    def one_head(h, carry):
        keys_t = jnp.concatenate([p[heads + h] for p in pieces], axis=1)
        keys = keys_t.T
        values = jnp.concatenate([p[2 * heads + h] for p in pieces], axis=1).T
        dkey = dvalue = None
        for b, gmix_ref in enumerate((gmix_a, gmix_b)):
            q_t = pieces[first + b][h]
            g_t = gmix_ref[h]
            probs = jnp.exp2(dot_nn(keys, q_t) * EXP_SCALE - lse_ref[h, b : b + 1])
            gprobs = dot_nn(values, g_t)
            inner = jnp.sum(probs * gprobs, axis=0, keepdims=True)
            gscores = (probs * (gprobs - inner)).astype(BF16)
            part_v = dot_nn(probs.astype(BF16), g_t.T)
            part_k = dot_nn(gscores, q_t.T)
            dvalue = part_v if dvalue is None else dvalue + part_v
            dkey = part_k if dkey is None else dkey + part_k
            dquery = (dot_nn(keys_t, gscores) * SCALE).astype(BF16)
            if last:
                outs[2 + b][h] = dquery
                outs[b][h] = dq_in[b][h]
            else:
                dq_outs[b][h] = dquery
        if last:
            dkey_t = ((dkey + acck_ref[h]) * SCALE).T.astype(BF16)
            dvalue_t = (dvalue + accv_ref[h]).T.astype(BF16)
            for p in range(4):
                outs[p][heads + h] = dkey_t[:, p * rows : (p + 1) * rows]
                outs[p][2 * heads + h] = dvalue_t[:, p * rows : (p + 1) * rows]
        else:
            dk_ref[h] = dkey
            dv_ref[h] = dvalue
        return carry

    lax.fori_loop(0, heads, one_head, 0)


def attn_bwd(pieces, first, lse, gmix, heads, carried=None):
    rows = pieces[0].shape[2]
    last = carried is not None
    vm = pl.BlockSpec(memory_space=pltpu.VMEM)
    if last:
        out_shape = (jax.ShapeDtypeStruct((3 * heads, HEAD, rows), BF16),) * 4
    else:
        out_shape = (jax.ShapeDtypeStruct((heads, HEAD, rows), BF16),) * 2 + (
            jax.ShapeDtypeStruct((heads, 4 * rows, HEAD), F32),
        ) * 2
    operands = (*pieces, lse, *gmix) + (tuple(carried) if last else ())
    return pl.pallas_call(
        functools.partial(attn_bwd_kernel, heads, first, last),
        out_shape=out_shape,
        in_specs=[vm] * len(operands),
        out_specs=[vm] * len(out_shape),
        compiler_params=pltpu.CompilerParams(vmem_limit_bytes=32 << 20),
        cost_estimate=cost(80 * heads * rows * rows * 128, 40 * rows * heads * HEAD, 8 * heads * rows * rows),
        name="attn_bwd",
    )(*operands)


def mlp_kernel(xa, xb, ga, gb, up_ref, bias_ref, down_ref, *outs):
    for x_ref, g_ref, (act_ref, ghid_ref, down_part_ref, in_part_ref) in (
        (xa, ga, outs[0::2]),
        (xb, gb, outs[1::2]),
    ):
        hidden = dot_nn(x_ref[...], up_ref[...]) + bias_ref[...]
        square = hidden * hidden
        tanh = jnp.tanh(GELU_C * hidden * (1.0 + 0.044715 * square))
        half_plus = 0.5 + 0.5 * tanh
        active = (hidden * half_plus).astype(BF16)
        slope = half_plus + 0.5 * hidden * (1.0 - tanh * tanh) * (
            GELU_C + (3.0 * 0.044715 * GELU_C) * square
        )
        act_ref[...] = active
        ghid = (dot_nt(g_ref[...], down_ref[...]) * slope).astype(BF16)
        ghid_ref[...] = ghid
        in_part_ref[...] = dot_nt(ghid, up_ref[...]).astype(BF16)
        down_part_ref[...] = dot_nn(active, down_ref[...]).astype(BF16)


def mlp(x, g, up, bias, down):
    rows, width = x[0].shape
    hid = up.shape[1]
    vm = pl.BlockSpec(memory_space=pltpu.VMEM)
    out = pl.pallas_call(
        mlp_kernel,
        out_shape=(jax.ShapeDtypeStruct((rows, hid), BF16),) * 4
        + (jax.ShapeDtypeStruct((rows, width), BF16),) * 4,
        in_specs=[vm] * 7,
        out_specs=[vm] * 8,
        compiler_params=pltpu.CompilerParams(vmem_limit_bytes=32 << 20),
        cost_estimate=cost(16 * rows * width * hid, 24 * rows * width + 4 * width * hid, 2 * rows * hid),
        name="mlp",
    )(*x, *g, up, bias, down)
    return tuple(out[2 * i : 2 * i + 2] for i in range(4))


def grad_kernel(by_rows, held_turned, bias_of_a, *refs):
    a_refs, b_refs = refs[:4], refs[4:8]
    err_ref, qt_ref, mat_ref, left_ref, bias_ref = refs[8:]
    step = pl.program_id(0)
    dot = dot_nn if held_turned else dot_tn
    mat = err_ref[...]
    for a_ref, b_ref in zip(a_refs, b_refs):
        mat = mat + dot(a_ref[...], b_ref[...])
    mat_ref[...] = mat
    high, low = split_low(mat)
    rank = qt_ref.shape[0]
    q_high, q_low = split_low(qt_ref[...])
    q_both = jnp.concatenate([q_high.astype(F32), q_low.astype(F32)], axis=0).astype(BF16)
    times = dot_nt if by_rows else dot_nn
    both = times(q_both, high)
    part = both[:rank] + (both[rank:] + times(q_high, low))
    if by_rows:
        left_ref[...] = part
    else:

        @pl.when(step == 0)
        def _():
            left_ref[...] = part

        @pl.when(step > 0)
        def _():
            left_ref[...] += part

    def token_sums():
        ones = jnp.ones((8, b_refs[0].shape[0]), BF16)
        total = 0.0
        for ref in a_refs if bias_of_a else b_refs:
            total = total + (dot_nt if bias_of_a else dot_nn)(ones, ref[...])
        bias_ref[...] = total

    if bias_of_a:
        token_sums()
    else:
        pl.when(step == 0)(token_sums)


def weight_grad(a, b, error, factor_t, by_rows, held_turned, bias_of_a, block):
    rows, cols = error.shape
    tokens = b[0].shape[0]
    rank = factor_t.shape[0]
    fixed = lambda i: (0, 0)
    row = lambda i: (i, 0)
    col = lambda i: (0, i)
    a_spec = pl.BlockSpec((block, tokens), row) if held_turned else pl.BlockSpec((tokens, block), col)
    if by_rows:
        left_len, left_spec = rows, pl.BlockSpec((rank, block), col)
        q_spec = pl.BlockSpec((rank, cols), fixed)
    else:
        left_len, left_spec = cols, pl.BlockSpec((rank, cols), fixed)
        q_spec = pl.BlockSpec((None, rank, block), lambda i: (i, 0, 0))
        factor_t = factor_t.reshape(rank, rows // block, block).swapaxes(0, 1) if factor_t.ndim == 2 else factor_t
        rank = factor_t.shape[1]
        left_spec = pl.BlockSpec((rank, cols), fixed)
        q_spec = pl.BlockSpec((None, rank, block), lambda i: (i, 0, 0))
    steps = rows // block
    if bias_of_a:
        bias_shape = (steps, 8, block)
        bias_spec = pl.BlockSpec((None, 8, block), lambda i: (i, 0, 0))
    else:
        bias_shape = (8, cols)
        bias_spec = pl.BlockSpec((8, cols), fixed)
    return pl.pallas_call(
        functools.partial(grad_kernel, by_rows, held_turned, bias_of_a),
        out_shape=(
            jax.ShapeDtypeStruct((rows, cols), F32),
            jax.ShapeDtypeStruct((rank, left_len), F32),
            jax.ShapeDtypeStruct(bias_shape, F32),
        ),
        grid=(steps,),
        in_specs=[a_spec] * 4
        + [pl.BlockSpec((tokens, cols), fixed, pipeline_mode=pl.Buffered(1))] * 4
        + [pl.BlockSpec((block, cols), row), q_spec],
        out_specs=[pl.BlockSpec((block, cols), row), left_spec, bias_spec],
        compiler_params=pltpu.CompilerParams(vmem_limit_bytes=28 << 20),
        cost_estimate=cost(8 * tokens * rows * cols, 8 * rows * cols + 8 * tokens * (rows + cols)),
        name="weight_grad",
    )(*a, *b, error, factor_t)


def orthonormal_rows(work):
    rank = work.shape[0]
    row = lax.broadcasted_iota(jnp.int32, (rank, 1), 0)
    for r in range(rank):
        vector = work[r : r + 1]
        unit = vector * lax.rsqrt(jnp.sum(vector * vector, axis=1, keepdims=True) + ORTH_EPS)
        dots = jnp.sum(work * unit, axis=1, keepdims=True)
        work = jnp.where(row > r, work - dots * unit, work)
        work = jnp.where(row == r, unit, work)
    return work


def stack_split(value):
    high, low = split_low(value)
    both = jnp.concatenate([high.astype(F32), low.astype(F32)], axis=0).astype(BF16)
    return high, both


def factor_kernel(dp_count, layouts, bias_lens, *refs):
    count = len(layouts)
    mats = refs[:count]
    lefts = refs[count : 2 * count]
    biases = refs[2 * count : 3 * count]
    second_ref, ortho_ref, bias_out = refs[3 * count : 3 * count + 3]
    scratch = refs[3 * count + 3 :]
    held = scratch[:count]
    pay_one, got_one, pay_two, got_two, in_sem, send_sem, recv_sem = scratch[count:]
    me = lax.axis_index("dp")
    rounds = dp_count.bit_length() - 1

    loads = [pltpu.make_async_copy(mats[i], held[i], in_sem.at[i]) for i in range(count)]
    for load in loads:
        load.start()

    barrier = pltpu.get_barrier_semaphore()
    for k in range(rounds):
        pl.semaphore_signal(barrier, inc=1, device_id={"dp": me ^ (1 << k)}, device_id_type=MESH)

    bias_row = RANK * count
    pay_one[bias_row:] = jnp.zeros_like(pay_one[bias_row:])
    for i in range(count):
        pay_one[RANK * i : RANK * (i + 1)] = lefts[i][...]
    for i in range(count):
        if len(biases[i].shape) == 3:
            for j in range(biases[i].shape[0]):
                where = bias_row + count + j
                pay_one[where : where + 1, : bias_lens[i]] = biases[i][j, 0:1]
        else:
            pay_one[bias_row + i : bias_row + i + 1, : bias_lens[i]] = biases[i][0:1]
    pl.semaphore_wait(barrier, rounds)

    def all_sum(payload, got, base):
        for k in range(rounds):
            copy = pltpu.make_async_remote_copy(
                src_ref=payload,
                dst_ref=got.at[k],
                send_sem=send_sem.at[base + k],
                recv_sem=recv_sem.at[base + k],
                device_id={"dp": me ^ (1 << k)},
                device_id_type=MESH,
            )
            copy.start()
            copy.wait()
            payload[...] += got[k]

    all_sum(pay_one, got_one, 0)
    bias_out[...] = pay_one[bias_row:]
    for i in range(count):
        ortho_ref[i] = orthonormal_rows(pay_one[RANK * i : RANK * (i + 1)])

    pay_two[...] = jnp.zeros_like(pay_two)
    for i, (kind, rows, block, offset) in enumerate(layouts):
        loads[i].wait()
        o_high, o_both = stack_split(ortho_ref[i])
        if kind:
            cols = held[i].shape[1]
            total = jnp.zeros((RANK, cols), F32)
            for b in range(rows // block):
                cut = slice(b * block, (b + 1) * block)
                high, low = split_low(held[i][cut])
                both = dot_nn(o_both[:, cut], high)
                total += both[:RANK] + (both[RANK:] + dot_nn(o_high[:, cut], low))
            pay_two[:, offset : offset + cols] = total
        else:
            step = block + (-block) % 128
            for b in range(rows // block):
                high, low = split_low(held[i][b * block : (b + 1) * block])
                both = dot_nt(o_both, high)
                part = both[:RANK] + (both[RANK:] + dot_nt(o_high, low))
                pay_two[:, offset + b * step : offset + b * step + block] = part

    all_sum(pay_two, got_two, rounds)
    second_ref[...] = pay_two[...] * (1.0 / dp_count)


def make_factors(mats, lefts, biases, layouts, wide):
    dp_count = lax.axis_size("dp")
    rounds = dp_count.bit_length() - 1
    count = len(mats)
    long = lefts[0].shape[1]
    pay_rows = RANK * count + 8
    bias_lens = tuple(b.shape[-1] for b in biases)
    vm = pl.BlockSpec(memory_space=pltpu.VMEM)
    hbm = pl.BlockSpec(memory_space=pl.ANY)
    return pl.pallas_call(
        functools.partial(factor_kernel, dp_count, layouts, bias_lens),
        out_shape=(
            jax.ShapeDtypeStruct((RANK, wide), F32),
            jax.ShapeDtypeStruct((count, RANK, long), F32),
            jax.ShapeDtypeStruct((8, long), F32),
        ),
        in_specs=[hbm] * count + [vm] * (2 * count),
        out_specs=[vm] * 3,
        scratch_shapes=[pltpu.VMEM(m.shape, F32) for m in mats]
        + [
            pltpu.VMEM((pay_rows, long), F32),
            pltpu.VMEM((rounds, pay_rows, long), F32),
            pltpu.VMEM((RANK, wide), F32),
            pltpu.VMEM((rounds, RANK, wide), F32),
            pltpu.SemaphoreType.DMA((count,)),
            pltpu.SemaphoreType.DMA((2 * rounds,)),
            pltpu.SemaphoreType.DMA((2 * rounds,)),
        ],
        compiler_params=pltpu.CompilerParams(
            collective_id=1, has_side_effects=True, vmem_limit_bytes=40 << 20
        ),
        cost_estimate=cost(4e9, 8 * sum(m.size for m in mats)),
        name="factors",
    )(*mats, *lefts, *biases)


def pack_three(value, first):
    high = value.astype(BF16).astype(F32)
    low = value - high
    parts = [high, high, low] if first else [high, low, high]
    return jnp.concatenate(parts, axis=0).astype(BF16)


def finish_kernel(layouts, own, *refs):
    count = len(layouts)
    mats = refs[:count]
    moments = refs[count : 2 * count]
    second_ref, ortho_ref = refs[2 * count : 2 * count + 2]
    outs = refs[2 * count + 2 :]
    rests, moments_next, updates = (outs[j * count : (j + 1) * count] for j in range(3))
    scratch = outs[3 * count :]
    held = scratch[:count]
    in_sem, out_sem = scratch[count:]
    me = lax.axis_index("dp")
    long = ortho_ref.shape[2]

    def block_of(ref, kind, b, block):
        return ref.at[:, pl.ds(b * block, block)] if kind else ref.at[pl.ds(b * block, block)]

    work = []
    for i, (kind, rows, block, offset) in enumerate(layouts):
        length = held[i].shape[1] if kind else rows
        for b in range(length // block):
            view = block_of(held[i], kind, b, block)
            load = pltpu.make_async_copy(block_of(mats[i], kind, b, block), view, in_sem.at[len(work)])
            load.start()
            work.append((i, kind, b, block, offset + b * (block + (-block) % 128), load, view))
    chosen = (
        lax.broadcasted_iota(jnp.int32, (long, own), 0)
        == lax.broadcasted_iota(jnp.int32, (long, own), 1) + me * own
    ).astype(F32).astype(BF16)
    stores = []
    packs = {}
    for n, (i, kind, b, block, offset, load, view) in enumerate(work):
        if i not in packs:
            pack = pack_three(ortho_ref[i], True)
            packs[i] = (pack, dot_nn(pack, chosen).astype(BF16))
        ortho_pack, own_pack = packs[i]
        second_pack = pack_three(second_ref[:, offset : offset + block], False)
        grad = dot_tn(own_pack, second_pack)
        if len(moments[i].shape) == 3:
            where = (b,)
        else:
            where = (slice(None), slice(b * block, (b + 1) * block))
        moment = MOMENTUM * moments[i][where] + grad
        moments_next[i][where] = moment
        updates[i][where] = -RATE * (grad + MOMENTUM * moment)
        load.wait()
        if kind:
            view[...] = view[...] - dot_tn(ortho_pack, second_pack)
        else:
            view[...] = view[...] - dot_tn(second_pack, ortho_pack)
        store = pltpu.make_async_copy(view, block_of(rests[i], kind, b, block), out_sem.at[n])
        store.start()
        stores.append(store)
    for store in stores:
        store.wait()


def finish(mats, moments, second, ortho, layouts):
    own = ortho.shape[2] // lax.axis_size("dp")
    count = len(mats)
    vm = pl.BlockSpec(memory_space=pltpu.VMEM)
    hbm = pl.BlockSpec(memory_space=pl.ANY)
    pieces = 16
    out = pl.pallas_call(
        functools.partial(finish_kernel, layouts, own),
        out_shape=tuple(
            [jax.ShapeDtypeStruct(m.shape, F32) for m in mats]
            + [jax.ShapeDtypeStruct(m.shape, F32) for m in moments] * 2
        ),
        in_specs=[hbm] * count + [vm] * (count + 2),
        out_specs=[hbm] * count + [vm] * (2 * count),
        scratch_shapes=[pltpu.VMEM(m.shape, F32) for m in mats]
        + [pltpu.SemaphoreType.DMA((pieces,)), pltpu.SemaphoreType.DMA((pieces,))],
        compiler_params=pltpu.CompilerParams(vmem_limit_bytes=40 << 20),
        cost_estimate=cost(4e9, 8 * sum(m.size for m in mats)),
        name="finish",
    )(*mats, *moments, second, ortho)
    return tuple(out[j * count : (j + 1) * count] for j in range(3))


def normalize(values):
    center = values - jnp.mean(values, axis=-1, keepdims=True)
    spread = jnp.mean(center * center, axis=-1, keepdims=True)
    inverse = lax.rsqrt(spread + EPS)
    return center * inverse, inverse


def normalize_back(grad, normed, inverse):
    return inverse * (
        grad
        - jnp.mean(grad, axis=-1, keepdims=True)
        - normed * jnp.mean(grad * normed, axis=-1, keepdims=True)
    )


def advance(moment, grad):
    moment_next = MOMENTUM * moment + grad
    return (moment_next, -RATE * (grad + MOMENTUM * moment_next))


def contract(a, b, left, right):
    return lax.dot_general(a, b, (((left,), (right,)), ((), ())), preferred_element_type=F32)


def per_device(
    tokens,
    modulation,
    qkv_weight,
    qv_bias,
    out_weight,
    out_bias,
    up_weight,
    up_bias,
    down_weight,
    down_bias,
    cotangent,
    qkv_factor,
    out_factor,
    up_factor,
    down_factor,
    qkv_error,
    out_error,
    up_error,
    down_error,
    qkv_moment,
    out_moment,
    up_moment,
    down_moment,
    qvbias_moment,
    outbias_moment,
    upbias_moment,
    downbias_moment,
):
    rows, width = tokens.shape[1:]
    local = qkv_weight.shape[2]
    hid = up_weight.shape[1]
    heads = local // HEAD
    dp_count = lax.axis_size("dp")
    shift_one, scale_one, gate_one, shift_two, scale_two, gate_two = (
        modulation[0, i : i + 1] for i in range(6)
    )
    token_vals = tokens[0].astype(F32)
    grad_final = cotangent[0].astype(F32)
    qkv_turned = qkv_weight.transpose(1, 2, 0).reshape(3 * local, width)
    bias_col = jnp.concatenate([qv_bias[0], jnp.zeros_like(qv_bias[0]), qv_bias[1]]).astype(F32)[:, None]

    def project(piece):
        value = (contract(qkv_turned, piece, 1, 1) + bias_col).astype(BF16)
        return value.reshape(3 * heads, HEAD, rows)

    def flat(piece):
        return piece.reshape(-1, rows)

    normed_one, inverse_one = normalize(token_vals)
    a_own = (normed_one * (1.0 + scale_one) + shift_one).astype(BF16)
    a_across = swap(a_own, 2)
    a_beside = swap(a_own, 1)
    qkv_own = project(a_own)
    qkv_beside = project(a_beside)
    a_across = after(a_across, qkv_beside)
    a_corner = swap(a_across, 1)
    g_own = (gate_two * grad_final).astype(BF16)
    g_source = after(g_own, a_across)
    g_across = swap(g_source, 2)
    g_beside = swap(g_source, 1)
    qkv_across = project(a_across)
    qkv_corner = project(a_corner)
    a_all = (a_own, a_beside, a_across, a_corner)
    qkv_all = (qkv_own, qkv_beside, qkv_across, qkv_corner)
    mix_across, mix_corner, lse_far = attn_fwd(qkv_all, 2, heads)

    def out_part(mix):
        return contract(flat(mix), out_weight, 0, 0).astype(BF16)

    out_sum = chip_sum(out_part(mix_across), out_part(mix_corner))
    out_across = swap(out_sum, 2)
    qkv_late = (after(qkv_own, out_sum),) + qkv_all[1:]
    mix_own, mix_beside, lse_near = attn_fwd(qkv_late, 0, heads)
    mix_all = (mix_own, mix_beside, mix_across, mix_corner)
    out_near = out_part(mix_own).astype(F32) + swap(out_part(mix_beside), 1).astype(F32)
    g_across = after(g_across, mix_own)
    g_corner = swap(g_across, 1)
    attn_out = out_near + out_across.astype(F32) + out_bias.astype(F32)
    middle = token_vals + gate_one * attn_out
    normed_two, inverse_two = normalize(middle)
    m_own = (normed_two * (1.0 + scale_two) + shift_two).astype(BF16)
    m_across = swap(m_own, 2)
    m_beside = swap(m_own, 1)

    up_bias_row = up_bias.astype(F32)[None]
    act_near, ghid_near, down_near, in_near = mlp(
        (m_own, m_beside), (g_own, g_beside), up_weight, up_bias_row, down_weight
    )
    m_across = after(m_across, act_near[0])
    m_corner = swap(m_across, 1)
    act_far, ghid_far, down_far, in_far = mlp(
        (m_across, m_corner), (g_across, g_corner), up_weight, up_bias_row, down_weight
    )
    m_all = (m_own, m_beside, m_across, m_corner)
    g_all = (g_own, g_beside, g_across, g_corner)
    in_sum = chip_sum(*in_far)
    in_across = swap(in_sum, 2)
    down_mat, down_left, downb = weight_grad(
        act_near + (after(act_far[0], in_sum), act_far[1]),
        g_all,
        down_error[0],
        down_factor.T,
        False,
        False,
        False,
        384,
    )
    up_mat, up_left, upb = weight_grad(
        m_all,
        ghid_near + (after(ghid_far[0], in_sum), ghid_far[1]),
        up_error[0],
        up_factor.T,
        True,
        False,
        False,
        384,
    )
    in_across = after(in_across, down_mat, up_mat)
    grad_mlp_in = in_near[0].astype(F32) + swap(in_near[1], 1).astype(F32) + in_across.astype(F32)
    grad_shift_two = jnp.sum(grad_mlp_in, axis=0)
    grad_scale_two = jnp.sum(grad_mlp_in * normed_two, axis=0)
    grad_middle = grad_final + normalize_back(grad_mlp_in * (1.0 + scale_two), normed_two, inverse_two)
    grad_gate_one = jnp.sum(grad_middle * attn_out, axis=0)
    b_own = (gate_one * grad_middle).astype(BF16)
    b_across = swap(b_own, 2)
    b_beside = swap(b_own, 1)

    def mix_grad(piece):
        return contract(out_weight, piece, 1, 1).astype(BF16).reshape(heads, HEAD, rows)

    carried = attn_bwd(qkv_all, 0, lse_near, (mix_grad(b_own), mix_grad(b_beside)), heads)
    b_across = after(b_across, carried[0])
    b_corner = swap(b_across, 1)
    b_all = (b_own, b_beside, b_across, b_corner)
    down_sum = chip_sum(after(down_far[0], b_across), down_far[1])
    mlp_across = swap(down_sum, 2)
    gp_all = attn_bwd(
        qkv_all,
        2,
        after(lse_far, down_sum),
        (mix_grad(b_across), mix_grad(b_corner)),
        heads,
        carried,
    )

    def back_part(piece):
        return contract(flat(piece), qkv_turned, 0, 0).astype(BF16)

    back_sum = chip_sum(back_part(gp_all[2]), back_part(gp_all[3]))
    back_across = swap(back_sum, 2)
    gp_late = (after(flat(gp_all[0]), back_sum),) + tuple(flat(p) for p in gp_all[1:])
    grad_attn_in = back_part(gp_all[0]).astype(F32) + swap(back_part(gp_all[1]), 1).astype(F32)
    out_mat, out_left, outb = weight_grad(
        tuple(flat(m) for m in mix_all), b_all, out_error[0], out_factor.T, False, True, False, local
    )
    qkv_mat, qkv_left, qvb = weight_grad(
        gp_late,
        a_all,
        qkv_error[0].transpose(1, 2, 0).reshape(3 * local, width),
        qkv_factor.transpose(0, 2, 1),
        False,
        True,
        True,
        local,
    )

    pad = local + (-local) % 128
    layouts = (
        (False, 3 * local, local, 0),
        (False, local, local, 3 * pad),
        (True, width, 384, 4 * pad),
        (False, hid, 384, 4 * pad + hid),
    )
    mats = (qkv_mat, out_mat, up_mat, down_mat)
    second, ortho, bias_sums = make_factors(
        mats, (qkv_left, out_left, up_left, down_left), (qvb, outb, upb, downb), layouts, 4 * pad + 2 * hid
    )

    mlp_out = (
        down_near[0].astype(F32)
        + swap(down_near[1], 1).astype(F32)
        + mlp_across.astype(F32)
        + down_bias.astype(F32)
    )
    tokens_out = (middle + gate_two * mlp_out).astype(BF16)
    grad_gate_two = jnp.sum(grad_final * mlp_out, axis=0)
    back_across = after(back_across, second)
    grad_attn_in = grad_attn_in + back_across.astype(F32)
    grad_shift_one = jnp.sum(grad_attn_in, axis=0)
    grad_scale_one = jnp.sum(grad_attn_in * normed_one, axis=0)
    tokens_grad = grad_middle + normalize_back(
        grad_attn_in * (1.0 + scale_one), normed_one, inverse_one
    )
    mod_part = jnp.stack(
        [grad_shift_one, grad_scale_one, grad_gate_one, grad_shift_two, grad_scale_two, grad_gate_two]
    )
    modulation_grad = mod_part + swap(mod_part, 1) + swap(mod_part, 2) + swap(mod_part, 3)

    moments = (qkv_moment.swapaxes(0, 1), out_moment.T, up_moment, down_moment.T)
    rests, moments_next, updates = finish(mats, moments, after(second, mod_part), ortho, layouts)

    bias_mean = bias_sums / dp_count
    qv_mean = jnp.stack([bias_mean[4, :local], bias_mean[6, :local]])
    qvbias_moment_next, qvbias_update = advance(qvbias_moment, qv_mean)
    outbias_moment_next, outbias_update = advance(outbias_moment, bias_mean[1])
    upbias_moment_next, upbias_update = advance(upbias_moment, bias_mean[2, :hid])
    downbias_moment_next, downbias_update = advance(downbias_moment, bias_mean[3])
    qkv_second = jnp.stack([second[:, k * pad : k * pad + local] for k in range(3)])
    return (
        tokens_out[None],
        tokens_grad[None],
        modulation_grad[None],
        qkv_second.transpose(0, 2, 1),
        rests[0].reshape(3, local, width).transpose(2, 0, 1)[None],
        moments_next[0].swapaxes(0, 1),
        updates[0].swapaxes(0, 1),
        second[:, 3 * pad : 3 * pad + local].T,
        rests[1][None],
        moments_next[1].T,
        updates[1].T,
        second[:, 4 * pad : 4 * pad + hid].T,
        rests[2][None],
        moments_next[2],
        updates[2],
        second[:, 4 * pad + hid :].T,
        rests[3][None],
        moments_next[3].T,
        updates[3].T,
        qvbias_moment_next,
        qvbias_update,
        outbias_moment_next,
        outbias_update,
        upbias_moment_next,
        upbias_update,
        downbias_moment_next,
        downbias_update,
    )


def solution(mesh):
    placed = (
        P("dp", "tensor", None),
        P("dp", None, None),
        P(None, None, "tensor"),
        P(None, "tensor"),
        P("tensor", None),
        P(),
        P(None, "tensor"),
        P("tensor"),
        P("tensor", None),
        P(),
        P("dp", "tensor", None),
        P(None, "tensor", None),
        P("tensor", None),
        P("tensor", None),
        P("tensor", None),
        P("dp", None, None, "tensor"),
        P("dp", "tensor", None),
        P("dp", None, "tensor"),
        P("dp", "tensor", None),
        P("dp", None, "tensor"),
        P("tensor", "dp"),
        P("dp", "tensor"),
        P("tensor", "dp"),
        P(None, "tensor"),
        P(),
        P("tensor"),
        P(),
    )
    return jax.shard_map(
        per_device,
        mesh=mesh,
        in_specs=placed,
        out_specs=(
            P("dp", "tensor", None),
            P("dp", "tensor", None),
            P("dp", None, None),
            P(None, "tensor", None),
            P("dp", None, None, "tensor"),
            P("dp", None, "tensor"),
            P("dp", None, "tensor"),
            P("tensor", None),
            P("dp", "tensor", None),
            P("tensor", "dp"),
            P("tensor", "dp"),
            P("tensor", None),
            P("dp", None, "tensor"),
            P("dp", "tensor"),
            P("dp", "tensor"),
            P("tensor", None),
            P("dp", "tensor", None),
            P("tensor", "dp"),
            P("tensor", "dp"),
            P(None, "tensor"),
            P(None, "tensor"),
            P(),
            P(),
            P("tensor"),
            P("tensor"),
            P(),
            P(),
        ),
        check_vma=False,
    )
```

```python
import functools

import jax
import jax.numpy as jnp
from jax import lax
from jax.experimental import pallas as pl
from jax.experimental.pallas import tpu as pltpu
from jax.sharding import PartitionSpec as P


HEAD = 72
RANK = 8
EPS = 1e-06
ORTH_EPS = 1e-06
MOMENTUM = 0.9
RATE = 0.01
F32 = jnp.float32
BF16 = jnp.bfloat16
MESH = pl.DeviceIdType.MESH
LOG2E = 1.4426950408889634
GELU_C = 0.7978845608028654


def dot_nn(a, b):
    return lax.dot_general(a, b, (((1,), (0,)), ((), ())), preferred_element_type=F32)


def dot_nt(a, b):
    return lax.dot_general(a, b, (((1,), (1,)), ((), ())), preferred_element_type=F32)


def dot_tn(a, b):
    return lax.dot_general(a, b, (((0,), (0,)), ((), ())), preferred_element_type=F32)


def split_low(value):
    high = value.astype(BF16)
    return high, (value - high.astype(F32)).astype(BF16)


def cost(flops, nbytes, trans=0):
    return pl.CostEstimate(flops=int(flops), bytes_accessed=int(nbytes), transcendentals=int(trans))


def swap(value, bit):
    size = lax.axis_size("tensor")
    return lax.ppermute(value, "tensor", [(i, i ^ bit) for i in range(size)])


def after(value, *others):
    return lax.optimization_barrier((value, *others))[0]


def chip_sum(part_across, part_corner):
    joined = swap(part_corner, 1)
    return (part_across.astype(F32) + joined.astype(F32)).astype(BF16)


SCALE = HEAD ** (-0.5)
EXP_SCALE = SCALE * LOG2E


def attn_fwd_kernel(heads, first, *refs):
    pieces, (mix_a, mix_b, lse_ref) = refs[:4], refs[4:]

    def one_head(h, carry):
        keys = jnp.concatenate([p[heads + h] for p in pieces], axis=1).T
        values_t = jnp.concatenate([p[2 * heads + h] for p in pieces], axis=1)
        for b, mix_ref in enumerate((mix_a, mix_b)):
            scores = dot_nn(keys, pieces[first + b][h])
            top = jnp.max(scores, axis=0, keepdims=True)
            expd = jnp.exp2((scores - top) * EXP_SCALE)
            total = jnp.sum(expd, axis=0, keepdims=True)
            probs = (expd * (1.0 / total)).astype(BF16)
            mix_ref[h] = dot_nn(values_t, probs).astype(BF16)
            lse_ref[h, b : b + 1] = top * EXP_SCALE + jnp.log2(total)
        return carry

    lax.fori_loop(0, heads, one_head, 0)


def attn_fwd(pieces, first, heads):
    rows = pieces[0].shape[2]
    vm = pl.BlockSpec(memory_space=pltpu.VMEM)
    return pl.pallas_call(
        functools.partial(attn_fwd_kernel, heads, first),
        out_shape=(
            jax.ShapeDtypeStruct((heads, HEAD, rows), BF16),
            jax.ShapeDtypeStruct((heads, HEAD, rows), BF16),
            jax.ShapeDtypeStruct((heads, 2, rows), F32),
        ),
        in_specs=[vm] * 4,
        out_specs=[vm] * 3,
        compiler_params=pltpu.CompilerParams(vmem_limit_bytes=12 << 20),
        cost_estimate=cost(32 * heads * rows * rows * 128, 16 * rows * heads * HEAD, 8 * heads * rows * rows),
        name="attn_fwd",
    )(*pieces)


def attn_bwd_kernel(heads, first, last, *refs):
    pieces = refs[:4]
    lse_ref, gmix_a, gmix_b = refs[4:7]
    rows = pieces[0].shape[2]
    if last:
        dq_in = refs[7:9]
        acck_ref, accv_ref = refs[9:11]
        outs = refs[11:]
    else:
        dq_outs = refs[7:9]
        dk_ref, dv_ref = refs[9:11]

    def one_head(h, carry):
        keys_t = jnp.concatenate([p[heads + h] for p in pieces], axis=1)
        keys = keys_t.T
        values = jnp.concatenate([p[2 * heads + h] for p in pieces], axis=1).T
        dkey = dvalue = None
        for b, gmix_ref in enumerate((gmix_a, gmix_b)):
            q_t = pieces[first + b][h]
            g_t = gmix_ref[h]
            probs = jnp.exp2(dot_nn(keys, q_t) * EXP_SCALE - lse_ref[h, b : b + 1])
            gprobs = dot_nn(values, g_t)
            inner = jnp.sum(probs * gprobs, axis=0, keepdims=True)
            gscores = (probs * (gprobs - inner)).astype(BF16)
            part_v = dot_nn(probs.astype(BF16), g_t.T)
            part_k = dot_nn(gscores, q_t.T)
            dvalue = part_v if dvalue is None else dvalue + part_v
            dkey = part_k if dkey is None else dkey + part_k
            dquery = (dot_nn(keys_t, gscores) * SCALE).astype(BF16)
            if last:
                outs[2 + b][h] = dquery
                outs[b][h] = dq_in[b][h]
            else:
                dq_outs[b][h] = dquery
        if last:
            dkey_t = ((dkey + acck_ref[h]) * SCALE).T.astype(BF16)
            dvalue_t = (dvalue + accv_ref[h]).T.astype(BF16)
            for p in range(4):
                outs[p][heads + h] = dkey_t[:, p * rows : (p + 1) * rows]
                outs[p][2 * heads + h] = dvalue_t[:, p * rows : (p + 1) * rows]
        else:
            dk_ref[h] = dkey
            dv_ref[h] = dvalue
        return carry

    lax.fori_loop(0, heads, one_head, 0)


def attn_bwd(pieces, first, lse, gmix, heads, carried=None):
    rows = pieces[0].shape[2]
    last = carried is not None
    vm = pl.BlockSpec(memory_space=pltpu.VMEM)
    if last:
        out_shape = (jax.ShapeDtypeStruct((3 * heads, HEAD, rows), BF16),) * 4
    else:
        out_shape = (jax.ShapeDtypeStruct((heads, HEAD, rows), BF16),) * 2 + (
            jax.ShapeDtypeStruct((heads, 4 * rows, HEAD), F32),
        ) * 2
    operands = (*pieces, lse, *gmix) + (tuple(carried) if last else ())
    return pl.pallas_call(
        functools.partial(attn_bwd_kernel, heads, first, last),
        out_shape=out_shape,
        in_specs=[vm] * len(operands),
        out_specs=[vm] * len(out_shape),
        compiler_params=pltpu.CompilerParams(vmem_limit_bytes=16 << 20),
        cost_estimate=cost(80 * heads * rows * rows * 128, 40 * rows * heads * HEAD, 8 * heads * rows * rows),
        name="attn_bwd",
    )(*operands)


def mlp_kernel(xa, xb, ga, gb, up_ref, bias_ref, down_ref, *rest):
    outs, (x_both, g_both) = rest[:8], rest[8:]
    x_both[0], x_both[1] = xa[...], xb[...]
    g_both[0], g_both[1] = ga[...], gb[...]

    def one_piece(i, carry):
        hidden = dot_nn(x_both[i], up_ref[...]) + bias_ref[...]
        square = hidden * hidden
        tanh = jnp.tanh(GELU_C * hidden * (1.0 + 0.044715 * square))
        half_plus = 0.5 + 0.5 * tanh
        active = (hidden * half_plus).astype(BF16)
        slope = half_plus + 0.5 * hidden * (1.0 - tanh * tanh) * (
            GELU_C + (3.0 * 0.044715 * GELU_C) * square
        )
        ghid = (dot_nt(g_both[i], down_ref[...]) * slope).astype(BF16)
        in_part = dot_nt(ghid, up_ref[...]).astype(BF16)
        down_part = dot_nn(active, down_ref[...]).astype(BF16)
        for which in range(2):

            @pl.when(i == which)
            def _():
                for ref, value in zip(outs[which::2], (active, ghid, down_part, in_part)):
                    ref[...] = value

        return carry

    lax.fori_loop(0, 2, one_piece, 0)


def mlp(x, g, up, bias, down):
    rows, width = x[0].shape
    hid = up.shape[1]
    vm = pl.BlockSpec(memory_space=pltpu.VMEM)
    out = pl.pallas_call(
        mlp_kernel,
        out_shape=(jax.ShapeDtypeStruct((rows, hid), BF16),) * 4
        + (jax.ShapeDtypeStruct((rows, width), BF16),) * 4,
        in_specs=[vm] * 7,
        out_specs=[vm] * 8,
        scratch_shapes=[pltpu.VMEM((2, rows, width), BF16)] * 2,
        compiler_params=pltpu.CompilerParams(vmem_limit_bytes=24 << 20),
        cost_estimate=cost(16 * rows * width * hid, 24 * rows * width + 4 * width * hid, 2 * rows * hid),
        name="mlp",
    )(*x, *g, up, bias, down)
    return tuple(out[2 * i : 2 * i + 2] for i in range(4))


def grad_kernel(by_rows, held_turned, bias_of_a, *refs):
    a_refs, b_refs = refs[:4], refs[4:8]
    err_ref, qt_ref, mat_ref, left_ref, bias_ref = refs[8:]
    step = pl.program_id(0)
    dot = dot_nn if held_turned else dot_tn
    mat = err_ref[...]
    for a_ref, b_ref in zip(a_refs, b_refs):
        mat = mat + dot(a_ref[...], b_ref[...])
    mat_ref[...] = mat
    high, low = split_low(mat)
    rank = qt_ref.shape[0]
    q_high, q_low = split_low(qt_ref[...])
    q_both = jnp.concatenate([q_high.astype(F32), q_low.astype(F32)], axis=0).astype(BF16)
    times = dot_nt if by_rows else dot_nn
    both = times(q_both, high)
    part = both[:rank] + (both[rank:] + times(q_high, low))
    if by_rows:
        left_ref[...] = part
    else:

        @pl.when(step == 0)
        def _():
            left_ref[...] = part

        @pl.when(step > 0)
        def _():
            left_ref[...] += part

    def token_sums():
        ones = jnp.ones((8, b_refs[0].shape[0]), BF16)
        total = 0.0
        for ref in a_refs if bias_of_a else b_refs:
            total = total + (dot_nt if bias_of_a else dot_nn)(ones, ref[...])
        bias_ref[...] = total

    if bias_of_a:
        token_sums()
    else:
        pl.when(step == 0)(token_sums)


def weight_grad(a, b, error, factor_t, by_rows, held_turned, bias_of_a, block):
    rows, cols = error.shape
    tokens = b[0].shape[0]
    rank = factor_t.shape[0]
    fixed = lambda i: (0, 0)
    row = lambda i: (i, 0)
    col = lambda i: (0, i)
    a_spec = pl.BlockSpec((block, tokens), row) if held_turned else pl.BlockSpec((tokens, block), col)
    if by_rows:
        left_len, left_spec = rows, pl.BlockSpec((rank, block), col)
        q_spec = pl.BlockSpec((rank, cols), fixed)
    else:
        left_len, left_spec = cols, pl.BlockSpec((rank, cols), fixed)
        q_spec = pl.BlockSpec((None, rank, block), lambda i: (i, 0, 0))
        factor_t = factor_t.reshape(rank, rows // block, block).swapaxes(0, 1) if factor_t.ndim == 2 else factor_t
        rank = factor_t.shape[1]
        left_spec = pl.BlockSpec((rank, cols), fixed)
        q_spec = pl.BlockSpec((None, rank, block), lambda i: (i, 0, 0))
    steps = rows // block
    if bias_of_a:
        bias_shape = (steps, 8, block)
        bias_spec = pl.BlockSpec((None, 8, block), lambda i: (i, 0, 0))
    else:
        bias_shape = (8, cols)
        bias_spec = pl.BlockSpec((8, cols), fixed)
    return pl.pallas_call(
        functools.partial(grad_kernel, by_rows, held_turned, bias_of_a),
        out_shape=(
            pltpu.HBM((rows, cols), F32),
            jax.ShapeDtypeStruct((rank, left_len), F32),
            jax.ShapeDtypeStruct(bias_shape, F32),
        ),
        grid=(steps,),
        in_specs=[a_spec] * 4
        + [pl.BlockSpec((tokens, cols), fixed, pipeline_mode=pl.Buffered(1))] * 4
        + [pl.BlockSpec((block, cols), row), q_spec],
        out_specs=[pl.BlockSpec((block, cols), row), left_spec, bias_spec],
        compiler_params=pltpu.CompilerParams(vmem_limit_bytes=20 << 20),
        cost_estimate=cost(8 * tokens * rows * cols, 8 * rows * cols + 8 * tokens * (rows + cols)),
        name="weight_grad",
    )(*a, *b, error, factor_t)


def orthonormal_rows(work):
    rank = work.shape[0]
    row = lax.broadcasted_iota(jnp.int32, (rank, 1), 0)
    for r in range(rank):
        vector = work[r : r + 1]
        unit = vector * lax.rsqrt(jnp.sum(vector * vector, axis=1, keepdims=True) + ORTH_EPS)
        dots = jnp.sum(work * unit, axis=1, keepdims=True)
        work = jnp.where(row > r, work - dots * unit, work)
        work = jnp.where(row == r, unit, work)
    return work


def stack_split(value):
    high, low = split_low(value)
    both = jnp.concatenate([high.astype(F32), low.astype(F32)], axis=0).astype(BF16)
    return high, both


def factor_kernel(dp_count, layouts, late, early_wide, *refs):
    count = len(layouts)
    mats = refs[:count]
    late_lefts = refs[count : count + late]
    early_left, qkv_bias, out_bias = refs[count + late : count + late + 3]
    second_ref, ortho_ref, bias_out = refs[count + late + 3 : count + late + 6]
    scratch = refs[count + late + 6 :]
    held = scratch[:count]
    pay_left, got_left, pay_bias, got_bias, pay_early, got_early, pay_late, got_late = scratch[count : count + 8]
    in_sem, send_sem, recv_sem = scratch[count + 8 :]
    me = lax.axis_index("dp")
    rounds = dp_count.bit_length() - 1

    loads = [pltpu.make_async_copy(mats[i], held[i], in_sem.at[i]) for i in range(count)]
    for i in (*range(late, count), *range(late)):
        loads[i].start()

    barrier = pltpu.get_barrier_semaphore()
    for k in range(rounds):
        pl.semaphore_signal(barrier, inc=1, device_id={"dp": me ^ (1 << k)}, device_id_type=MESH)
    for i in range(late):
        pay_left[RANK * i : RANK * (i + 1)] = late_lefts[i][...]
    pay_bias[...] = jnp.zeros_like(pay_bias)
    local = qkv_bias.shape[2]
    for k in range(3):
        start = k * (local + (-local) % 128)
        pay_bias[0:1, start : start + local] = qkv_bias[k, 0:1]
    pay_bias[1:2] = out_bias[0:1]
    pay_early[...] = jnp.zeros_like(pay_early)
    pay_late[...] = jnp.zeros_like(pay_late)
    pl.semaphore_wait(barrier, rounds)

    class Sum:
        def __init__(self, base, payload, got):
            self.base, self.payload, self.got, self.k = base, payload, got, 0

        def start(self):
            k = self.k
            self.copy = pltpu.make_async_remote_copy(
                src_ref=self.payload,
                dst_ref=self.got.at[k],
                send_sem=send_sem.at[self.base * rounds + k],
                recv_sem=recv_sem.at[self.base * rounds + k],
                device_id={"dp": me ^ (1 << k)},
                device_id_type=MESH,
            )
            self.copy.start()

        def end(self):
            self.copy.wait()
            self.payload[...] += self.got[self.k]
            self.k += 1

    left_sum = Sum(0, pay_left, got_left)
    bias_sum = Sum(1, pay_bias, got_bias)
    early_sum = Sum(2, pay_early, got_early)
    late_sum = Sum(3, pay_late, got_late)

    def right_factor(i):
        kind, rows, block, offset = layouts[i]
        target, offset = (pay_late, offset - early_wide) if i < late else (pay_early, offset)
        loads[i].wait()
        o_high, o_both = stack_split(ortho_ref[i])
        if kind:
            cols = held[i].shape[1]
            total = jnp.zeros((RANK, cols), F32)
            for b in range(rows // block):
                cut = slice(b * block, (b + 1) * block)
                high, low = split_low(held[i][cut])
                both = dot_nn(o_both[:, cut], high)
                total += both[:RANK] + (both[RANK:] + dot_nn(o_high[:, cut], low))
            target[:, offset : offset + cols] = total
        else:
            step = block + (-block) % 128
            for b in range(rows // block):
                high, low = split_low(held[i][b * block : (b + 1) * block])
                both = dot_nt(o_both, high)
                part = both[:RANK] + (both[RANK:] + dot_nt(o_high, low))
                target[:, offset + b * step : offset + b * step + block] = part

    def left_round(meanwhile):
        left_sum.start()
        bias_sum.start()
        meanwhile()
        left_sum.end()
        bias_sum.end()

    def early_orthos():
        for i in range(late, count):
            ortho_ref[i] = orthonormal_rows(early_left[RANK * (i - late) : RANK * (i - late + 1)])

    def early_rights():
        for i in range(late, count):
            right_factor(i)

    left_round(early_orthos)
    left_round(early_rights)
    early_sum.start()
    for _ in range(2, rounds):
        left_round(lambda: None)
    early_sum.end()
    early_sum.start()
    bias_out[...] = pay_bias[...]
    for i in range(late):
        ortho_ref[i] = orthonormal_rows(pay_left[RANK * i : RANK * (i + 1)])
    for i in range(late):
        right_factor(i)
    late_sum.start()
    early_sum.end()
    for _ in range(2, rounds):
        early_sum.start()
        late_sum.end()
        late_sum.start()
        early_sum.end()
    late_sum.end()
    late_sum.start()
    late_sum.end()
    second_ref[:, :early_wide] = pay_early[...] * (1.0 / dp_count)
    second_ref[:, early_wide:] = pay_late[...] * (1.0 / dp_count)


def make_factors(mats, late_lefts, early_left, qkv_bias, out_bias, layouts, early_wide, wide):
    dp_count = lax.axis_size("dp")
    rounds = dp_count.bit_length() - 1
    count = len(mats)
    late = len(late_lefts)
    long = early_left.shape[1]
    vm = pl.BlockSpec(memory_space=pltpu.VMEM)
    hbm = pl.BlockSpec(memory_space=pltpu.HBM)
    payloads = []
    for shape in ((RANK * late, long), (2, long), (RANK, early_wide), (RANK, wide - early_wide)):
        payloads += [pltpu.VMEM(shape, F32), pltpu.VMEM((rounds, *shape), F32)]
    return pl.pallas_call(
        functools.partial(factor_kernel, dp_count, layouts, late, early_wide),
        out_shape=(
            jax.ShapeDtypeStruct((RANK, wide), F32),
            jax.ShapeDtypeStruct((count, RANK, long), F32),
            jax.ShapeDtypeStruct((2, long), F32),
        ),
        in_specs=[hbm] * count + [vm] * (late + 3),
        out_specs=[vm] * 3,
        scratch_shapes=[pltpu.VMEM(m.shape, F32) for m in mats]
        + payloads
        + [
            pltpu.SemaphoreType.DMA((count,)),
            pltpu.SemaphoreType.DMA((4 * rounds,)),
            pltpu.SemaphoreType.DMA((4 * rounds,)),
        ],
        compiler_params=pltpu.CompilerParams(
            collective_id=1, has_side_effects=True, vmem_limit_bytes=24 << 20
        ),
        cost_estimate=cost(8e9, 8 * sum(m.size for m in mats)),
        name="factors",
    )(*mats, *late_lefts, early_left, qkv_bias, out_bias)


def pack_three(value, first):
    high = value.astype(BF16).astype(F32)
    low = value - high
    parts = [high, high, low] if first else [high, low, high]
    return jnp.concatenate(parts, axis=0).astype(BF16)


def finish_kernel(layouts, own, *refs):
    count = len(layouts)
    mats = refs[:count]
    moments = refs[count : 2 * count]
    second_ref, ortho_ref = refs[2 * count : 2 * count + 2]
    outs = refs[2 * count + 2 :]
    rests, moments_next, updates, seconds = (outs[j * count : (j + 1) * count] for j in range(4))
    scratch = outs[4 * count :]
    held, held_moment, held_update = (scratch[j * count : (j + 1) * count] for j in range(3))
    in_sem, out_sem, moment_sem = scratch[3 * count :]
    me = lax.axis_index("dp")
    long = ortho_ref.shape[2]

    def block_of(ref, kind, b, block):
        return ref.at[:, pl.ds(b * block, block)] if kind else ref.at[pl.ds(b * block, block)]

    moment_loads = []
    for i in range(count):
        load = pltpu.make_async_copy(moments[i], held_moment[i], moment_sem.at[i])
        load.start()
        moment_loads.append(load)
    work = []
    for i, (kind, rows, block, offset) in enumerate(layouts):
        length = held[i].shape[1] if kind else rows
        for b in range(length // block):
            view = block_of(held[i], kind, b, block)
            load = pltpu.make_async_copy(block_of(mats[i], kind, b, block), view, in_sem.at[len(work)])
            load.start()
            work.append((i, kind, b, block, offset + b * (block + (-block) % 128), load, view))
    chosen = (
        lax.broadcasted_iota(jnp.int32, (long, own), 0)
        == lax.broadcasted_iota(jnp.int32, (long, own), 1) + me * own
    ).astype(F32).astype(BF16)
    packs = []
    for i in range(count):
        pack = pack_three(ortho_ref[i], True)
        packs.append((pack, dot_nn(pack, chosen).astype(BF16)))
    stores = []
    for n, (i, kind, b, block, offset, load, view) in enumerate(work):
        second = second_ref[:, offset : offset + block]
        second_pack = pack_three(second, False)
        load.wait()
        if kind:
            view[...] = view[...] - dot_tn(packs[i][0], second_pack)
        else:
            view[...] = view[...] - dot_tn(second_pack, packs[i][0])
        store = pltpu.make_async_copy(view, block_of(rests[i], kind, b, block), out_sem.at[n])
        store.start()
        stores.append(store)
        grad = dot_tn(packs[i][1], second_pack)
        three = len(moments[i].shape) == 3
        where = (b,) if three else (slice(None), slice(b * block, (b + 1) * block))
        if b == 0:
            moment_loads[i].wait()
        moment = MOMENTUM * held_moment[i][where] + grad
        held_moment[i][where] = moment
        held_update[i][where] = -RATE * (grad + MOMENTUM * moment)
        if three:
            seconds[i][b] = second
        else:
            seconds[i][:, b * block : (b + 1) * block] = second
        if n + 1 == len(work) or work[n + 1][0] != i:
            for j, (source, target) in enumerate(
                ((held_moment[i], moments_next[i]), (held_update[i], updates[i]))
            ):
                store = pltpu.make_async_copy(source, target, moment_sem.at[count * (j + 1) + i])
                store.start()
                stores.append(store)
    for store in stores:
        store.wait()


def finish(mats, moments, second, ortho, layouts):
    own = ortho.shape[2] // lax.axis_size("dp")
    count = len(mats)
    vm = pl.BlockSpec(memory_space=pltpu.VMEM)
    hbm = pl.BlockSpec(memory_space=pltpu.HBM)
    pieces = sum((m.shape[1] if kind else rows) // block for m, (kind, rows, block, _) in zip(mats, layouts))
    second_shapes = [
        (m.shape[0], RANK, m.shape[2]) if m.ndim == 3 else (RANK, m.shape[1]) for m in moments
    ]
    out = pl.pallas_call(
        functools.partial(finish_kernel, layouts, own),
        out_shape=tuple(
            [jax.ShapeDtypeStruct(m.shape, F32) for m in mats]
            + [jax.ShapeDtypeStruct(m.shape, F32) for m in moments] * 2
            + [jax.ShapeDtypeStruct(shape, F32) for shape in second_shapes]
        ),
        in_specs=[hbm] * (2 * count) + [vm] * 2,
        out_specs=[hbm] * (3 * count) + [vm] * count,
        scratch_shapes=[pltpu.VMEM(m.shape, F32) for m in mats]
        + [pltpu.VMEM(m.shape, F32) for m in moments] * 2
        + [
            pltpu.SemaphoreType.DMA((pieces,)),
            pltpu.SemaphoreType.DMA((pieces,)),
            pltpu.SemaphoreType.DMA((3 * count,)),
        ],
        compiler_params=pltpu.CompilerParams(vmem_limit_bytes=26 << 20),
        cost_estimate=cost(8e9, 8 * sum(m.size for m in mats)),
        name="finish",
    )(*mats, *moments, second, ortho)
    return tuple(out[j * count : (j + 1) * count] for j in range(4))


def norm_back_kernel(gated, *refs):
    part_a, part_b, part_c, value_ref, base_ref, scale_ref = refs[:6]
    if gated:
        branch_ref, gate_ref, out_ref, sums_ref, gated_ref = refs[6:]
    else:
        out_ref, sums_ref = refs[6:]
    rows, width = value_ref.shape
    chunk = 32
    inverse_width = 1.0 / width

    def fold(value):
        return jnp.sum(value.reshape(chunk // 8, 8, width), axis=0)

    def one_chunk(i, sums):
        cut = pl.ds(pl.multiple_of(i * chunk, chunk), chunk)
        grad = part_a[cut].astype(F32) + part_b[cut].astype(F32) + part_c[cut].astype(F32)
        value = value_ref[cut].astype(F32)
        center = value - jnp.sum(value, axis=1, keepdims=True) * inverse_width
        spread = jnp.sum(center * center, axis=1, keepdims=True) * inverse_width
        inverse = lax.rsqrt(spread + EPS)
        normed = center * inverse
        scaled = grad * (1.0 + scale_ref[...])
        mean_one = jnp.sum(scaled, axis=1, keepdims=True) * inverse_width
        mean_two = jnp.sum(scaled * normed, axis=1, keepdims=True) * inverse_width
        out = base_ref[cut].astype(F32) + inverse * (scaled - mean_one - normed * mean_two)
        out_ref[cut] = out
        new = [sums[0] + fold(grad), sums[1] + fold(grad * normed)]
        if gated:
            new.append(sums[2] + fold(out * branch_ref[cut]))
            gated_ref[cut] = (gate_ref[...] * out).astype(BF16)
        return tuple(new)

    zero = jnp.zeros((8, width), F32)
    sums = lax.fori_loop(0, rows // chunk, one_chunk, (zero,) * (3 if gated else 2))
    for i, total in enumerate(sums):
        sums_ref[i : i + 1] = jnp.sum(total, axis=0, keepdims=True)


def norm_back(parts, value, base, scale, branch=None, gate=None):
    rows, width = value.shape
    gated = branch is not None
    operands = (*parts, value, base, scale) + ((branch, gate) if gated else ())
    vm = pl.BlockSpec(memory_space=pltpu.VMEM)
    out_shape = (
        jax.ShapeDtypeStruct((rows, width), F32),
        jax.ShapeDtypeStruct((3 if gated else 2, width), F32),
    ) + ((jax.ShapeDtypeStruct((rows, width), BF16),) if gated else ())
    return pl.pallas_call(
        functools.partial(norm_back_kernel, gated),
        out_shape=out_shape,
        in_specs=[vm] * len(operands),
        out_specs=[vm] * len(out_shape),
        compiler_params=pltpu.CompilerParams(vmem_limit_bytes=8 << 20),
        cost_estimate=cost(40 * rows * width, 24 * rows * width),
        name="norm_back",
    )(*operands)


def normalize(values):
    center = values - jnp.mean(values, axis=-1, keepdims=True)
    spread = jnp.mean(center * center, axis=-1, keepdims=True)
    inverse = lax.rsqrt(spread + EPS)
    return center * inverse, inverse


def advance(moment, grad):
    moment_next = MOMENTUM * moment + grad
    return (moment_next, -RATE * (grad + MOMENTUM * moment_next))


def contract(a, b, left, right):
    return lax.dot_general(a, b, (((left,), (right,)), ((), ())), preferred_element_type=F32)


def per_device(
    tokens,
    modulation,
    qkv_weight,
    qv_bias,
    out_weight,
    out_bias,
    up_weight,
    up_bias,
    down_weight,
    down_bias,
    cotangent,
    qkv_factor,
    out_factor,
    up_factor,
    down_factor,
    qkv_error,
    out_error,
    up_error,
    down_error,
    qkv_moment,
    out_moment,
    up_moment,
    down_moment,
    qvbias_moment,
    outbias_moment,
    upbias_moment,
    downbias_moment,
):
    rows, width = tokens.shape[1:]
    local = qkv_weight.shape[2]
    hid = up_weight.shape[1]
    heads = local // HEAD
    dp_count = lax.axis_size("dp")
    shift_one, scale_one, gate_one, shift_two, scale_two, gate_two = (
        modulation[0, i : i + 1] for i in range(6)
    )
    token_vals = tokens[0].astype(F32)
    grad_final = cotangent[0].astype(F32)
    qkv_turned = qkv_weight.transpose(1, 2, 0).reshape(3 * local, width)
    bias_col = jnp.concatenate([qv_bias[0], jnp.zeros_like(qv_bias[0]), qv_bias[1]]).astype(F32)[:, None]

    def project(piece):
        value = (contract(qkv_turned, piece, 1, 1) + bias_col).astype(BF16)
        return value.reshape(3 * heads, HEAD, rows)

    def flat(piece):
        return piece.reshape(-1, rows)

    normed_one, _ = normalize(token_vals)
    a_own = (normed_one * (1.0 + scale_one) + shift_one).astype(BF16)
    a_across = swap(a_own, 2)
    a_beside = swap(a_own, 1)
    qkv_own = project(a_own)
    qkv_beside = project(a_beside)
    a_across = after(a_across, qkv_beside)
    a_corner = swap(a_across, 1)
    g_own = (gate_two * grad_final).astype(BF16)
    g_source = after(g_own, a_across)
    g_across = swap(g_source, 2)
    g_beside = swap(g_source, 1)
    qkv_across = project(a_across)
    qkv_corner = project(a_corner)
    a_all = (a_own, a_beside, a_across, a_corner)
    qkv_all = (qkv_own, qkv_beside, qkv_across, qkv_corner)
    mix_across, mix_corner, lse_far = attn_fwd(qkv_all, 2, heads)

    def out_part(mix):
        return contract(flat(mix), out_weight, 0, 0).astype(BF16)

    out_sum = chip_sum(out_part(mix_across), out_part(mix_corner))
    out_across = swap(out_sum, 2)
    qkv_late = (after(qkv_own, out_sum, g_across),) + qkv_all[1:]
    mix_own, mix_beside, lse_near = attn_fwd(qkv_late, 0, heads)
    mix_all = (mix_own, mix_beside, mix_across, mix_corner)
    out_near = out_part(mix_own).astype(F32) + swap(out_part(mix_beside), 1).astype(F32)
    g_corner = swap(g_across, 1)
    attn_out = out_near + out_across.astype(F32) + out_bias.astype(F32)
    middle = token_vals + gate_one * attn_out
    normed_two, _ = normalize(middle)
    m_own = (normed_two * (1.0 + scale_two) + shift_two).astype(BF16)
    m_across = swap(m_own, 2)
    m_beside = swap(m_own, 1)

    up_bias_row = up_bias.astype(F32)[None]
    act_near, ghid_near, down_near, in_near = mlp(
        (m_own, m_beside), (g_own, g_beside), up_weight, up_bias_row, down_weight
    )
    m_across = after(m_across, act_near[0])
    m_corner = swap(m_across, 1)
    act_far, ghid_far, down_far, in_far = mlp(
        (m_across, m_corner), (g_across, g_corner), up_weight, up_bias_row, down_weight
    )
    m_all = (m_own, m_beside, m_across, m_corner)
    g_all = (g_own, g_beside, g_across, g_corner)
    in_sum = chip_sum(*in_far)
    in_across = swap(in_sum, 2)
    down_mat, down_left, downb = weight_grad(
        act_near + (after(act_far[0], in_sum), act_far[1]),
        g_all,
        down_error[0],
        down_factor.T,
        False,
        False,
        False,
        384,
    )
    up_mat, up_left, upb = weight_grad(
        m_all,
        ghid_near + (after(ghid_far[0], in_sum), ghid_far[1]),
        up_error[0],
        up_factor.T,
        True,
        False,
        False,
        384,
    )
    early = jnp.concatenate([up_left, down_left, upb[:4], downb[:4]], axis=0)
    in_across = after(in_across, down_mat, up_mat)
    grad_middle, mid_sums, b_own = norm_back(
        (in_near[0], swap(in_near[1], 1), in_across),
        middle,
        cotangent[0],
        scale_two,
        attn_out,
        gate_one,
    )
    rounds = dp_count.bit_length() - 1

    def dp_round(value, k):
        other = lax.ppermute(value, "dp", [(i, i ^ (1 << k)) for i in range(dp_count)])
        return value + other

    b_across = swap(b_own, 2)
    b_beside = swap(b_own, 1)

    def mix_grad(piece):
        return contract(out_weight, piece, 1, 1).astype(BF16).reshape(heads, HEAD, rows)

    carried = attn_bwd(qkv_all, 0, lse_near, (mix_grad(b_own), mix_grad(b_beside)), heads)
    early = dp_round(early, 0)
    for k in range(1, rounds - 2):
        early = dp_round(early, k)
    early = after(early, carried[0])
    early_next = dp_round(early, rounds - 2)
    b_across = after(b_across, carried[0])
    b_corner = swap(b_across, 1)
    b_all = (b_own, b_beside, b_across, b_corner)
    down_sum = chip_sum(after(down_far[0], b_across), down_far[1])
    mlp_across = swap(down_sum, 2)
    gp_all = attn_bwd(
        qkv_all,
        2,
        after(lse_far, down_sum),
        (mix_grad(b_across), mix_grad(b_corner)),
        heads,
        carried,
    )

    def back_part(piece):
        return contract(flat(piece), qkv_turned, 0, 0).astype(BF16)

    back_sum = chip_sum(back_part(gp_all[2]), back_part(gp_all[3]))
    early = dp_round(after(early_next, gp_all[2]), rounds - 1)
    back_across = swap(back_sum, 2)
    gp_late = (after(flat(gp_all[0]), back_sum),) + tuple(flat(p) for p in gp_all[1:])
    back_own, back_beside = back_part(gp_all[0]), swap(back_part(gp_all[1]), 1)
    out_mat, out_left, outb = weight_grad(
        tuple(flat(m) for m in mix_all), b_all, out_error[0], out_factor.T, False, True, False, local
    )
    qkv_mat, qkv_left, qvb = weight_grad(
        gp_late,
        a_all,
        qkv_error[0].transpose(1, 2, 0).reshape(3 * local, width),
        qkv_factor.transpose(0, 2, 1),
        False,
        True,
        True,
        local,
    )

    pad = local + (-local) % 128
    layouts = (
        (False, 3 * local, local, 2 * hid),
        (False, local, local, 2 * hid + 3 * pad),
        (True, width, 384, 0),
        (False, hid, 384, hid),
    )
    mats = (qkv_mat, out_mat, up_mat, down_mat)
    second, ortho, late_bias = make_factors(
        mats, (qkv_left, out_left), early, qvb, outb, layouts, 2 * hid, 2 * hid + 4 * pad
    )

    mlp_out = (
        down_near[0].astype(F32)
        + swap(down_near[1], 1).astype(F32)
        + mlp_across.astype(F32)
        + down_bias.astype(F32)
    )
    tokens_out = (middle + gate_two * mlp_out).astype(BF16)
    grad_gate_two = jnp.sum(grad_final * mlp_out, axis=0)
    back_across = after(back_across, second)
    tokens_grad, end_sums = norm_back(
        (back_own, back_beside, back_across), tokens[0], grad_middle, scale_one
    )
    mod_part = jnp.concatenate(
        [end_sums, mid_sums[2:3], mid_sums[0:2], grad_gate_two[None]], axis=0
    )
    modulation_grad = mod_part + swap(mod_part, 1) + swap(mod_part, 2) + swap(mod_part, 3)

    moments = (qkv_moment.swapaxes(0, 1), out_moment.T, up_moment, down_moment.T)
    rests, moments_next, updates, seconds = finish(mats, moments, after(second, mod_part), ortho, layouts)

    qv_mean = jnp.stack([late_bias[0, :local], late_bias[0, 2 * pad : 2 * pad + local]]) / dp_count
    qvbias_moment_next, qvbias_update = advance(qvbias_moment, qv_mean)
    outbias_moment_next, outbias_update = advance(outbias_moment, late_bias[1] / dp_count)
    upbias_moment_next, upbias_update = advance(upbias_moment, early[2 * RANK, :hid] / dp_count)
    downbias_moment_next, downbias_update = advance(downbias_moment, early[2 * RANK + 4] / dp_count)
    return (
        tokens_out[None],
        tokens_grad[None],
        modulation_grad[None],
        seconds[0].transpose(0, 2, 1),
        rests[0].reshape(3, local, width).transpose(2, 0, 1)[None],
        moments_next[0].swapaxes(0, 1),
        updates[0].swapaxes(0, 1),
        seconds[1].T,
        rests[1][None],
        moments_next[1].T,
        updates[1].T,
        seconds[2].T,
        rests[2][None],
        moments_next[2],
        updates[2],
        seconds[3].T,
        rests[3][None],
        moments_next[3].T,
        updates[3].T,
        qvbias_moment_next,
        qvbias_update,
        outbias_moment_next,
        outbias_update,
        upbias_moment_next,
        upbias_update,
        downbias_moment_next,
        downbias_update,
    )


def solution(mesh):
    placed = (
        P("dp", "tensor", None),
        P("dp", None, None),
        P(None, None, "tensor"),
        P(None, "tensor"),
        P("tensor", None),
        P(),
        P(None, "tensor"),
        P("tensor"),
        P("tensor", None),
        P(),
        P("dp", "tensor", None),
        P(None, "tensor", None),
        P("tensor", None),
        P("tensor", None),
        P("tensor", None),
        P("dp", None, None, "tensor"),
        P("dp", "tensor", None),
        P("dp", None, "tensor"),
        P("dp", "tensor", None),
        P("dp", None, "tensor"),
        P("tensor", "dp"),
        P("dp", "tensor"),
        P("tensor", "dp"),
        P(None, "tensor"),
        P(),
        P("tensor"),
        P(),
    )

    return jax.shard_map(
        per_device,
        mesh=mesh,
        in_specs=placed,
        out_specs=(
            P("dp", "tensor", None),
            P("dp", "tensor", None),
            P("dp", None, None),
            P(None, "tensor", None),
            P("dp", None, None, "tensor"),
            P("dp", None, "tensor"),
            P("dp", None, "tensor"),
            P("tensor", None),
            P("dp", "tensor", None),
            P("tensor", "dp"),
            P("tensor", "dp"),
            P("tensor", None),
            P("dp", None, "tensor"),
            P("dp", "tensor"),
            P("dp", "tensor"),
            P("tensor", None),
            P("dp", "tensor", None),
            P("tensor", "dp"),
            P("tensor", "dp"),
            P(None, "tensor"),
            P(None, "tensor"),
            P(),
            P(),
            P("tensor"),
            P("tensor"),
            P(),
            P(),
        ),
        check_vma=False,
    )
```
